32 devices in a mesh: dom: 8 (over y, x, core), band: 4 (over z).
Axes of the slice: x: 2, y: 2, z: 4, core: 2. Of those that a mesh axis runs over, the one named last changes fastest.
Arguments:
- wavefunctions: bfloat16 [4096, 512], P('dom', 'band'), may hold values from -6 to 6
- cell_ham: bfloat16 [16, 512, 512], P('dom'), may hold values from -0.25 to 0.25
- connectivity: int32 [16, 512], P('dom'), may hold values from 0 to 767, as said below
- inv_mass: float32 [4096], P('dom'), may hold values from 0.5 to 2
- cell_count: int32 [8], P('dom'), may hold values from 1 to 2, as said below
Outputs:
- filtered: bfloat16 [4096, 512], P('dom', 'band')
- margin: float32 [512, 512], P('band', 'dom')
The draws below stay inside these ranges and needn't reach their ends.
Inputs may be any that keep to these rules, and one draw needn't show every extreme that they name: `connectivity`: row c of domain d lists 512 indices into that domain's nodes extended by 128 nodes on each side; every extended index appears in some row of its domain. `cell_count`: some domain has all 2 cells live in every draw.
All inputs are finite; a program needn't handle non-finite values.
Results may differ from the reference program's by a relative error of at most 0.0052.
Values may be sent and summed in bfloat16 or wider, within the bound.
No kernel may reach another device: no remote copies, remote signals or barrier semaphores. Data moves between devices by JAX's collectives and lax.ppermute only.
A program may use at most 64 MiB of HBM per device.

```python
import math
import jax
import jax.numpy as jnp
from jax import lax

NPC = 512
CELLS_DEV = 2
DEGREE = 4
NODES_DEV = 512
GHOST = 128
NODES = 4096
CELLS = 16
NBANDS = 512
N_DOM = 8


def draw_connectivity(key, part):
    domains = CELLS // CELLS_DEV
    extended = NODES_DEV + 2 * GHOST
    slots = CELLS_DEV * NPC

    def single(subkey):
        first, second, third = jax.random.split(subkey, 3)
        base = jax.random.permutation(first, extended)
        extra = jax.random.randint(second, (slots - extended,), 0, extended)
        joined = jnp.concatenate([base, extra])
        joined = jax.random.permutation(third, joined)
        return joined.reshape(CELLS_DEV, NPC)
    keys = jax.random.split(jax.random.fold_in(key, 11), domains)
    return jax.vmap(single)(keys).reshape(CELLS, NPC).astype(jnp.int32)


def draw_cell_count(key, part):
    domains = NODES // NODES_DEV
    first, second = jax.random.split(jax.random.fold_in(key, 23))
    lowest = max(1, CELLS_DEV // 2)
    counts = jax.random.randint(first, (domains,), lowest, CELLS_DEV + 1)
    chosen = jax.random.randint(second, (), 0, domains)
    counts = jnp.where(jnp.arange(domains) == chosen, CELLS_DEV, counts)
    return counts.astype(jnp.int32)


def levels(rng, shape, cuts, low, largest):
    def one(position, shards_of):
        steps = jax.random.uniform(jax.random.fold_in(jax.random.fold_in(rng, 6), position), (shards_of,), jnp.float32, low / len(cuts), largest / len(cuts))
        return jnp.repeat(jnp.exp(steps), shape[position] // shards_of).reshape((-1,) + (1,) * (len(shape) - position - 1))

    factor_of = one(*cuts[0])
    for cut in cuts[1:]:
        factor_of = factor_of * one(*cut)
    return factor_of


def normal_values(key, dims, scale, limit, cuts=(), held_as=jnp.bfloat16):
    factor_of = levels(key, dims, cuts, -0.22, 0.18) if cuts else 1.0
    values = jax.random.normal(key, dims, jnp.float32) * scale * factor_of
    return jnp.minimum(jnp.maximum(values, -limit), limit).astype(held_as)


def setup_inputs(seed: int = 0) -> dict:
    seeds = jax.random.split(jax.random.key(seed), 6)
    return {
        "wavefunctions": normal_values(seeds[0], (NODES, NBANDS), 1.0, 6.0, ((0, 8), (1, 4))),
        "cell_ham": normal_values(seeds[1], (CELLS, NPC, NPC), NPC ** -0.5, 0.25, ((0, 8),)),
        "connectivity": draw_connectivity(jax.random.fold_in(seeds[5], 71), 0),
        "inv_mass": jnp.clip(jnp.exp(math.log(2.0) - 1.3862944 * jax.random.uniform(seeds[3], (NODES,), jnp.float32) ** levels(seeds[3], (NODES,), ((0, 8),), -0.2, 0.2)), 0.5, 2.0),
        "cell_count": draw_cell_count(jax.random.fold_in(seeds[5], 71), 0),
    }


filter_center = 0.5
filter_halfwidth = 3.0

def apply_operator(current, cell_ham, connectivity, inv_mass, cell_count):
    values = current.astype(jnp.bfloat16)

    def per_domain(total, domain):
        hams = lax.dynamic_slice_in_dim(cell_ham, domain * CELLS_DEV, CELLS_DEV, 0)
        conn = lax.dynamic_slice_in_dim(connectivity, domain * CELLS_DEV, CELLS_DEV, 0)
        glob = jnp.mod(domain * NODES_DEV + conn - GHOST, NODES).astype(jnp.int32)
        taken = values[glob]
        prod = jnp.einsum('cij,cjb->cib', hams.astype(jnp.float32), taken.astype(jnp.float32))
        live = (jnp.arange(CELLS_DEV, dtype=jnp.int32) < cell_count[domain]).astype(jnp.float32)
        prod = prod * live[:, None, None]
        total = total.at[glob.reshape(-1)].add(prod.reshape(-1, prod.shape[-1]))
        return (total, None)
    start = jnp.zeros(current.shape, jnp.float32)
    total, unused = lax.scan(per_domain, start, jnp.arange(N_DOM, dtype=jnp.int32))
    return inv_mass[:, None] * total

def reference(wavefunctions, cell_ham, connectivity, inv_mass, cell_count):

    def operate(field):
        return apply_operator(field, cell_ham, connectivity, inv_mass, cell_count)
    previous = wavefunctions.astype(jnp.float32)
    current = (operate(previous) - filter_center * previous) / filter_halfwidth
    for step in range(DEGREE - 1):
        following = 2.0 * (operate(current) - filter_center * current) / filter_halfwidth - previous
        previous = current
        current = following
    filtered = current.astype(jnp.bfloat16)
    gram = jnp.dot(filtered.T, filtered, preferred_element_type=jnp.float32)
    margin = gram * (1.0 / jnp.sqrt(jnp.float32(NODES)))
    return (filtered, margin)
```

```python
import functools

import jax
import jax.numpy as jnp
from jax import lax
from jax.experimental import pallas as pl
from jax.experimental.pallas import tpu as pltpu
from jax.sharding import PartitionSpec as P

DEGREE = 4
LANES = 128
PAD = 16
VMEM_LIMIT = 16 << 20

filter_center = 0.5
filter_halfwidth = 3.0

F32 = jnp.float32
BF16 = jnp.bfloat16
VMEM = pl.BlockSpec(memory_space=pltpu.VMEM)
SMEM = pl.BlockSpec(memory_space=pltpu.SMEM)


def call(kernel, name, outs, ins, flops, scratch=()):
    return pl.pallas_call(
        kernel,
        name=name,
        out_shape=[jax.ShapeDtypeStruct(s, d) for s, d in outs],
        in_specs=ins,
        out_specs=[VMEM] * len(outs),
        scratch_shapes=list(scratch),
        cost_estimate=pl.CostEstimate(flops=flops, bytes_accessed=1 << 20, transcendentals=0),
        compiler_params=pltpu.CompilerParams(vmem_limit_bytes=VMEM_LIMIT),
    )


def rows_to_columns(row):
    width = row.shape[1]
    parts = [
        jnp.broadcast_to(row[:, i : i + LANES], (LANES, LANES)).T for i in range(0, width, LANES)
    ]
    return parts[0] if len(parts) == 1 else jnp.concatenate(parts, axis=0)


def assemble_kernel(pos_ref, ham_ref, k_ref):
    ext = k_ref.shape[0]
    cells, slots = pos_ref.shape
    total = None
    for c in range(cells):
        row = pos_ref[c : c + 1, :]
        spread = lax.broadcasted_iota(jnp.int32, (ext, slots), 0) == row
        spread = jnp.where(spread, 1.0, 0.0).astype(BF16)
        rows = jnp.dot(spread, ham_ref[c], preferred_element_type=F32).astype(BF16)
        column = rows_to_columns(row.astype(F32)).astype(jnp.int32)
        lane = lax.broadcasted_iota(jnp.int32, (slots, LANES), 1)
        pick = jnp.concatenate(
            [
                jnp.where(lane + i == column, 1.0, 0.0).astype(BF16)
                for i in range(0, ext, LANES)
            ],
            axis=1,
        )
        part = jnp.dot(rows, pick, preferred_element_type=F32)
        total = part if total is None else total + part
    k_ref[...] = total.astype(BF16)


def at(start, size):
    return pl.ds(pl.multiple_of(start, LANES), size)


def multiply(k_ref, values, p_ref, se_ref, so_ref, odd, last):
    product = jnp.dot(k_ref[...], values, preferred_element_type=F32)
    p_ref[...] = product
    ext = product.shape[0]
    size = se_ref.shape[0]
    if last:
        so_ref[...] = p_ref[at(jnp.where(odd, size, 0), size), :].astype(BF16)
        se_ref[...] = p_ref[at(ext - 2 * size + jnp.where(odd, 0, size), size), :].astype(BF16)
    else:
        so_ref[...] = product[:size].astype(BF16)
        se_ref[...] = product[ext - size :].astype(BF16)


def first_kernel(odd_ref, v_ref, he_ref, ho_ref, d_ref, k_ref, vx_ref, c_ref, p_ref, se_ref, so_ref):
    odd = odd_ref[0] == 1
    owned = v_ref.shape[0]
    ext = k_ref.shape[0]
    g = (ext - owned) // 2
    base = ext - 2 * g
    far = owned - g

    def mass(ref):
        return rows_to_columns(jnp.sum(ref[g:, :].astype(F32), axis=0, keepdims=True))

    def own_mass(block):
        return rows_to_columns(d_ref[pl.ds(block, 1), :])

    ho_at = at(jnp.where(odd, g, 0), g)
    oo_at = at(jnp.where(odd, 0, g), g)
    he_at = at(base + jnp.where(odd, 0, g), g)
    oe_at = at(base + jnp.where(odd, g, 0), g)
    vx_ref[ho_at, :] = ho_ref[:g, :]
    vx_ref[oo_at, :] = v_ref[at(jnp.where(odd, far, 0), g), :]
    vx_ref[2 * g : base, :] = v_ref[g : owned - g, :]
    vx_ref[he_at, :] = he_ref[:g, :]
    vx_ref[oe_at, :] = v_ref[at(jnp.where(odd, 0, far), g), :]
    c_ref[ho_at, :] = mass(ho_ref)
    c_ref[oo_at, :] = own_mass(jnp.where(odd, far // LANES, 0))
    for i in range(1, far // LANES):
        c_ref[g + i * LANES : g + (i + 1) * LANES, :] = own_mass(i)
    c_ref[he_at, :] = mass(he_ref)
    c_ref[oe_at, :] = own_mass(jnp.where(odd, 0, far // LANES))
    multiply(k_ref, vx_ref[...], p_ref, se_ref, so_ref, odd, False)


def advance(applied, current, previous):
    moved = (applied - filter_center * current) / filter_halfwidth
    return moved if previous is None else 2.0 * moved - previous


def step_kernel(first, last, odd_ref, re_ref, ro_ref, p_ref, c_ref, y_ref, *rest):
    rest = list(rest)
    prev_ref = None if first else rest.pop(0)
    k_ref, y_out, p_out, se_ref, so_ref = rest
    ext = p_ref.shape[0]
    size = re_ref.shape[0]
    for start, stop, extra in (
        (0, size, ro_ref),
        (size, ext - size, None),
        (ext - size, ext, re_ref),
    ):
        total = p_ref[start:stop, :]
        if extra is not None:
            total = total + extra[...].astype(F32)
        y_out[start:stop, :] = advance(
            c_ref[start:stop, :] * total,
            y_ref[start:stop, :].astype(F32),
            None if first else prev_ref[start:stop, :].astype(F32),
        )
    multiply(k_ref, y_out[...].astype(BF16), p_out, se_ref, so_ref, odd_ref[0] == 1, last)


def last_kernel(odd_ref, re_ref, ro_ref, p_ref, c_ref, y_ref, prev_ref, f_ref):
    odd = odd_ref[0] == 1
    ext = p_ref.shape[0]
    owned = f_ref.shape[0]
    g = re_ref.shape[0]
    base = ext - 2 * g

    def piece(src, extra):
        total = p_ref[src, :]
        if extra is not None:
            total = total + extra[...].astype(F32)
        return advance(c_ref[src, :] * total, y_ref[src, :], prev_ref[src, :]).astype(BF16)

    far = owned - g
    f_ref[g:far, :] = piece(slice(2 * g, base), None)
    f_ref[at(jnp.where(odd, far, 0), g), :] = piece(at(jnp.where(odd, 0, g), g), ro_ref)
    f_ref[at(jnp.where(odd, 0, far), g), :] = piece(at(base + jnp.where(odd, g, 0), g), re_ref)


def margin_kernel(bands, mine_ref, own_ref, *refs):
    out_ref = refs[-1]
    own = own_ref[...]
    width = own.shape[1]
    for k in range(bands):
        other = own if k == 0 else refs[k - 1][...]
        block = lax.dot_general(other, own, (((0,), (0,)), ((), ())), preferred_element_type=F32)
        out_ref[at((mine_ref[0] ^ k) * width, width), :] = block.astype(BF16)


def shards(wavefunctions, cell_ham, connectivity, inv_mass, cell_count):
    owned, width = wavefunctions.shape
    cells, slots = connectivity.shape
    g = cell_ham.shape[1] // 4
    ext = owned + 2 * g
    base = ext - 2 * g
    domains = lax.axis_size("dom")
    bands = lax.axis_size("band")
    if domains % 2 or bands & (bands - 1) or g != LANES or width != LANES:
        raise ValueError("unsupported sizes")
    me = lax.axis_index("dom")
    odd = jnp.mod(me, 2).astype(jnp.int32)
    odd_ref = odd.reshape(1)
    even_pairs = [(i, i ^ 1) for i in range(domains)]
    odd_pairs = [(i, (i + 1) % domains if i % 2 else (i - 1) % domains) for i in range(domains)]

    def swap_even(x):
        return lax.ppermute(x, "dom", even_pairs)

    def swap_odd(x):
        return lax.ppermute(x, "dom", odd_pairs)

    masses = inv_mass.reshape(owned // LANES, LANES)
    high = inv_mass.astype(BF16)
    low = (inv_mass - high.astype(F32)).astype(BF16)

    def rim(start):
        values = lax.dynamic_slice_in_dim(wavefunctions, start, g, 0)
        pair = [lax.dynamic_slice_in_dim(m, start, g, 0)[None] for m in (high, low)]
        return jnp.concatenate([values] + pair + [jnp.zeros((PAD - 2, g), BF16)], 0)

    halo_o = swap_odd(rim(odd * (owned - g)))
    halo_e = swap_even(rim((1 - odd) * (owned - g)))

    flipped = jnp.where(
        connectivity < 2 * g,
        connectivity + base,
        jnp.where(connectivity >= base, connectivity - base, connectivity),
    )
    position = jnp.where(odd == 1, flipped, connectivity)
    live = lax.broadcasted_iota(jnp.int32, (cells, slots), 0) < cell_count[0]
    position = jnp.where(live, position, -1)

    (operator,) = call(
        assemble_kernel,
        "assemble",
        [((ext, ext), BF16)],
        [VMEM, VMEM],
        2 * cells * ext * slots * (slots + ext),
    )(position, cell_ham)

    block = ((2 * g, width), BF16)
    half = ((g, width), BF16)
    full = ((ext, width), F32)
    flops = 2 * ext * ext * width
    current, scale, product, to_e, to_o = call(
        first_kernel,
        "first",
        [((ext, width), BF16), full, full, block, block],
        [SMEM] + [VMEM] * 5,
        flops,
    )(odd_ref, wavefunctions, halo_e, halo_o, masses, operator)

    previous = None
    for step in range(DEGREE - 1):
        last = step == DEGREE - 2
        from_o = swap_odd(to_o)
        from_e = swap_even(to_e)
        history = [current] if previous is None else [current, previous]
        following, product, to_e, to_o = call(
            functools.partial(step_kernel, previous is None, last),
            "step",
            [full, full] + [half if last else block] * 2,
            [SMEM] + [VMEM] * (5 + len(history)),
            flops,
        )(odd_ref, from_e, from_o, product, scale, *history, operator)
        previous = current
        current = following
    from_o = swap_odd(to_o)
    from_e = swap_even(to_e)
    if previous.dtype != F32:
        previous = previous.astype(F32)
    (filtered,) = call(
        last_kernel,
        "last",
        [((owned, width), BF16)],
        [SMEM] + [VMEM] * 6,
        owned * width * 8,
    )(odd_ref, from_e, from_o, product, scale, current, previous)

    others = [
        lax.ppermute(filtered, "band", [(i, i ^ k) for i in range(bands)]) for k in range(1, bands)
    ]
    mine = lax.axis_index("band").astype(jnp.int32).reshape(1)
    total = bands * width
    (sums,) = call(
        functools.partial(margin_kernel, bands),
        "margin",
        [((total, width), BF16)],
        [SMEM] + [VMEM] * bands,
        2 * total * width * owned,
    )(mine, filtered, *others)
    parts = lax.all_to_all(sums.reshape(domains, total // domains, width), "dom", 0, 0)
    factor = 1.0 / jnp.sqrt(F32(owned * domains))
    return (filtered, (jnp.sum(parts.astype(F32), axis=0) * factor).T)


def solution(mesh):
    return jax.shard_map(
        shards,
        mesh=mesh,
        in_specs=(P("dom", "band"), P("dom", None, None), P("dom", None), P("dom"), P("dom")),
        out_specs=(P("dom", "band"), P("band", "dom")),
        check_vma=False,
    )
```

```python
import functools

import jax
import jax.numpy as jnp
from jax import lax
from jax.experimental import pallas as pl
from jax.experimental.pallas import tpu as pltpu
from jax.sharding import PartitionSpec as P


DEGREE = 4
LANES = 128
PAD = 16
VMEM_LIMIT = 16 << 20

filter_center = 0.5
filter_halfwidth = 3.0

F32 = jnp.float32
BF16 = jnp.bfloat16
VMEM = pl.BlockSpec(memory_space=pltpu.VMEM)
SMEM = pl.BlockSpec(memory_space=pltpu.SMEM)
HBM = pl.BlockSpec(memory_space=pltpu.HBM)


def call(kernel, outs, ins, flops, scratch=()):
    return pl.pallas_call(
        kernel,
        out_shape=[jax.ShapeDtypeStruct(s, d) for s, d in outs],
        in_specs=ins,
        out_specs=[VMEM] * len(outs),
        scratch_shapes=list(scratch),
        cost_estimate=pl.CostEstimate(flops=flops, bytes_accessed=1 << 20, transcendentals=0),
        compiler_params=pltpu.CompilerParams(vmem_limit_bytes=VMEM_LIMIT),
    )


def is_odd():
    return jnp.bitwise_and(lax.axis_index("dom"), 1) == 1


def at(start, size):
    return pl.ds(pl.multiple_of(start, LANES), size)


def to_columns(row):
    width = row.shape[1]
    parts = [
        jnp.broadcast_to(row[:, i : i + LANES], (LANES, LANES)).T for i in range(0, width, LANES)
    ]
    return parts[0] if len(parts) == 1 else jnp.concatenate(parts, axis=0)


def split(x):
    high = x.astype(BF16)
    return high, (x - high.astype(F32)).astype(BF16)


def dot(a, b):
    return jnp.dot(a, b, preferred_element_type=F32)


def apply(hi_ref, lo_ref, rows, cols, values):
    return dot(hi_ref[rows, cols], values) + dot(lo_ref[rows, cols], values)


def advance(applied, current, previous):
    moved = (applied - filter_center * current) / filter_halfwidth
    return moved if previous is None else 2.0 * moved - previous


def rim_kernel(
    count_ref, v_hbm, d_hbm, conn_hbm, ham_hbm, ro_ref, re_ref, v_ref, d_ref, pos_ref, ham_ref, sems
):
    pairs = (
        (ham_hbm, ham_ref),
        (v_hbm, v_ref),
        (d_hbm, d_ref),
        (conn_hbm, pos_ref),
    )
    copies = [pltpu.make_async_copy(a, b, sems.at[i]) for i, (a, b) in enumerate(pairs)]
    for copy in copies[1:] + copies[:1]:
        copy.start()
    odd = is_odd()
    owned = v_ref.shape[0]
    g = ro_ref.shape[0] - PAD
    far = owned - g
    row = lax.broadcasted_iota(jnp.int32, (PAD, LANES), 0)
    for copy in copies[1:]:
        copy.wait()
    for out, edge in ((ro_ref, jnp.where(odd, far, 0)), (re_ref, jnp.where(odd, 0, far))):
        out[:g, :] = v_ref[at(edge, g), :]
        mass = d_ref[pl.ds(edge // LANES, 1), :]
        high = mass.astype(BF16).astype(F32)
        out[g:, :] = jnp.where(row == 0, high, jnp.where(row == 1, mass - high, 0.0)).astype(BF16)
    cells, slots = pos_ref.shape
    edge = slots // 2
    base = owned + 2 * g - edge
    conn = pos_ref[...]
    turned = jnp.where(conn < edge, conn + base, jnp.where(conn >= base, conn - base, conn))
    live = lax.broadcasted_iota(jnp.int32, (cells, slots), 0) < count_ref[0]
    pos_ref[...] = jnp.where(live, jnp.where(odd, turned, conn), -1)
    copies[0].wait()


def assemble_kernel(pos_ref, ham_ref, hi_ref, lo_ref):
    ext = hi_ref.shape[0]
    cells, slots = pos_ref.shape
    total = None
    for c in range(cells):
        row = pos_ref[c : c + 1, :]
        spread = lax.broadcasted_iota(jnp.int32, (ext, slots), 0) == row
        spread = jnp.where(spread, 1.0, 0.0).astype(BF16)
        high, low = split(dot(spread, ham_ref[c]))
        column = to_columns(row.astype(F32)).astype(jnp.int32)
        lane = lax.broadcasted_iota(jnp.int32, (slots, LANES), 1)
        pick = jnp.concatenate(
            [jnp.where(lane + i == column, 1.0, 0.0).astype(BF16) for i in range(0, ext, LANES)],
            axis=1,
        )
        part = dot(high, pick) + dot(low, pick)
        total = part if total is None else total + part
    hi_ref[...], lo_ref[...] = split(total)


def first_o_kernel(v_ref, he_ref, ho_ref, hi_ref, lo_ref, vx_ref, p_ref, s_ref):
    odd = is_odd()
    owned = v_ref.shape[0]
    ext = hi_ref.shape[0]
    g = (ext - owned) // 2
    base = ext - 2 * g
    far = owned - g
    vx_ref[at(jnp.where(odd, g, 0), g), :] = ho_ref[:g, :]
    vx_ref[at(jnp.where(odd, 0, g), g), :] = v_ref[at(jnp.where(odd, far, 0), g), :]
    vx_ref[2 * g : base, :] = v_ref[g:far, :]
    vx_ref[at(base + jnp.where(odd, 0, g), g), :] = he_ref[:g, :]
    vx_ref[at(base + jnp.where(odd, g, 0), g), :] = v_ref[at(jnp.where(odd, 0, far), g), :]
    product = apply(hi_ref, lo_ref, slice(0, 2 * g), slice(None), vx_ref[...])
    p_ref[...] = product
    s_ref[...] = product.astype(BF16)


def first_e_kernel(vx_ref, he_ref, ho_ref, d_ref, hi_ref, lo_ref, c_ref, p_ref, y_ref, v_ref):
    odd = is_odd()
    ext = hi_ref.shape[0]
    g = he_ref.shape[0] - PAD
    owned = ext - 2 * g
    base = ext - 2 * g
    far = owned - g

    def mass(ref):
        return to_columns(jnp.sum(ref[g:, :].astype(F32), axis=0, keepdims=True))

    def own(block):
        return to_columns(d_ref[pl.ds(block, 1), :])

    c_ref[at(jnp.where(odd, g, 0), g), :] = mass(ho_ref)
    c_ref[at(jnp.where(odd, 0, g), g), :] = own(jnp.where(odd, far // LANES, 0))
    for i in range(1, far // LANES):
        c_ref[g + i * LANES : g + (i + 1) * LANES, :] = own(i)
    c_ref[at(base + jnp.where(odd, 0, g), g), :] = mass(he_ref)
    c_ref[at(base + jnp.where(odd, g, 0), g), :] = own(jnp.where(odd, 0, far // LANES))
    product = apply(hi_ref, lo_ref, slice(2 * g, ext), slice(None), vx_ref[...])
    p_ref[...] = product[base - 2 * g :]
    middle = slice(2 * g, base)
    y = advance(c_ref[middle, :] * product[: base - 2 * g], vx_ref[middle, :].astype(F32), None)
    y_ref[...] = y
    v_ref[...] = y.astype(BF16)


def middle_kernel(edge, v_ref, hi_ref, lo_ref, part_ref):
    ext = hi_ref.shape[0]
    part_ref[...] = apply(hi_ref, lo_ref, slice(None), slice(edge, ext - edge), v_ref[...])


def even_kernel(r_ref, p_ref, c_ref, y_ref, prev_ref, part_ref, hi_ref, lo_ref, y_out, po_out, pe_out):
    ext = hi_ref.shape[0]
    edge = r_ref.shape[0]
    block = slice(ext - edge, ext)
    y = advance(c_ref[block, :] * (p_ref[...] + r_ref[...]), y_ref[...], prev_ref[...])
    y_out[...] = y
    part = part_ref[...] + apply(hi_ref, lo_ref, slice(None), block, y.astype(BF16))
    po_out[...] = part[:edge]
    pe_out[...] = part[edge:]


def even_first_kernel(r_ref, p_ref, c_ref, vx_ref, part_ref, hi_ref, lo_ref, y_out, po_out, pe_out):
    ext = hi_ref.shape[0]
    edge = r_ref.shape[0]
    block = slice(ext - edge, ext)
    y = advance(c_ref[block, :] * (p_ref[...] + r_ref[...]), vx_ref[block, :].astype(F32), None)
    y_out[...] = y
    part = part_ref[...] + apply(hi_ref, lo_ref, slice(None), block, y.astype(BF16))
    po_out[...] = part[:edge]
    pe_out[...] = part[edge:]


def odd_kernel(first, last, r_ref, p_ref, c_ref, y_ref, *rest):
    rest = list(rest)
    prev_ref = None if first else rest.pop(0)
    part_ref, hi_ref, lo_ref, y_out, v_out, p_out, s_out = rest
    edge = r_ref.shape[0]
    block = slice(0, edge)
    y = advance(
        c_ref[block, :] * (p_ref[...] + r_ref[...].astype(F32)),
        y_ref[block, :].astype(F32),
        None if first else prev_ref[block, :].astype(F32),
    )
    y_out[...] = y
    values = y.astype(BF16)
    v_out[...] = values
    product = part_ref[...] + apply(hi_ref, lo_ref, block, block, values)
    p_out[...] = product
    if last:
        g = s_out.shape[0]
        s_out[...] = p_out[at(jnp.where(is_odd(), g, 0), g), :].astype(BF16)
    else:
        s_out[...] = product.astype(BF16)


def rest_kernel(last, v_ref, part_ref, c_ref, y_ref, prev_ref, hi_ref, lo_ref, p_out, *outs):
    ext = hi_ref.shape[0]
    edge = v_ref.shape[0]
    base = ext - edge
    product = part_ref[...] + apply(hi_ref, lo_ref, slice(edge, ext), slice(0, edge), v_ref[...])
    p_out[...] = product[base - edge :]
    middle = slice(edge, base)
    y = advance(
        c_ref[middle, :] * product[: base - edge],
        y_ref[...],
        prev_ref[middle, :].astype(F32) if prev_ref.shape[0] == ext else prev_ref[...],
    )
    if last:
        f_out, s_out = outs
        f_out[...] = y.astype(BF16)
        g = s_out.shape[0]
        s_out[...] = p_out[at(jnp.where(is_odd(), 0, g), g), :]
    else:
        y_out, v_out = outs
        y_out[...] = y
        v_out[...] = y.astype(BF16)


def last_kernel(re_ref, ro_ref, pe_ref, po_ref, c_ref, ye_ref, yo_ref, we_ref, wo_ref, f_ref):
    odd = is_odd()
    ext = c_ref.shape[0]
    g = re_ref.shape[0]
    base = ext - 2 * g
    here = at(jnp.where(odd, 0, g), g)
    total = po_ref[here, :] + ro_ref[...].astype(F32)
    f_ref[:g, :] = advance(c_ref[here, :] * total, yo_ref[here, :], wo_ref[here, :]).astype(BF16)
    here = at(jnp.where(odd, g, 0), g)
    total = pe_ref[here, :] + re_ref[...]
    scale = c_ref[at(base + jnp.where(odd, g, 0), g), :]
    f_ref[g:, :] = advance(scale * total, ye_ref[here, :], we_ref[here, :]).astype(BF16)


def join_kernel(fm_ref, fb_ref, out_ref):
    odd = is_odd()
    g = fb_ref.shape[0] // 2
    far = out_ref.shape[0] - g
    out_ref[g:far, :] = fm_ref[...]
    out_ref[at(jnp.where(odd, far, 0), g), :] = fb_ref[:g, :]
    out_ref[at(jnp.where(odd, 0, far), g), :] = fb_ref[g:, :]


def margin_kernel(bands, start, *refs):
    refs = list(refs)
    before = None if start else refs.pop(0)
    out_ref = refs.pop()
    own = refs[0][...]
    width = own.shape[1]
    for k in range(bands):
        other = own if k == 0 else refs[k][...]
        block = lax.dot_general(other, own, (((0,), (0,)), ((), ())), preferred_element_type=F32)
        place = at((lax.axis_index("band") ^ k) * width, width)
        if start:
            out_ref[place, :] = block
        else:
            out_ref[place, :] = (before[place, :] + block).astype(BF16)


def shards(wavefunctions, cell_ham, connectivity, inv_mass, cell_count):
    owned, width = wavefunctions.shape
    cells, slots = connectivity.shape
    g = cell_ham.shape[1] // 4
    edge = 2 * g
    ext = owned + edge
    inner = ext - 2 * edge
    domains = lax.axis_size("dom")
    bands = lax.axis_size("band")
    if domains % 2 or bands & (bands - 1) or g != LANES or width != LANES or slots != 2 * edge:
        raise ValueError("unsupported sizes")
    even_pairs = [(i, i ^ 1) for i in range(domains)]
    odd_pairs = [(i, (i + 1) % domains if i % 2 else (i - 1) % domains) for i in range(domains)]

    def swap_even(x):
        return lax.ppermute(x, "dom", even_pairs)

    def swap_odd(x):
        return lax.ppermute(x, "dom", odd_pairs)

    def spread(x):
        out = []
        for k in range(1, bands):
            out.append(lax.ppermute(x, "band", [(i, i ^ k) for i in range(bands)]))
        return out

    def flops(rows, cols):
        return 4 * rows * cols * width

    masses = inv_mass.reshape(owned // LANES, LANES)
    rim = ((g + PAD, width), BF16)
    inputs = (wavefunctions, masses, connectivity, cell_ham)
    rim_o, rim_e, wavefunctions, masses, position, cell_ham = call(
        rim_kernel,
        [rim, rim] + [(x.shape, x.dtype) for x in inputs],
        [SMEM] + [HBM] * 4,
        1 << 10,
        [pltpu.SemaphoreType.DMA((4,))],
    )(cell_count, *[pltpu.with_memory_space_constraint(x, pltpu.HBM) for x in inputs])
    halo_o = swap_odd(rim_o)
    halo_e = swap_even(rim_e)
    square = ((ext, ext), BF16)
    operator = call(
        assemble_kernel, [square, square], [VMEM, VMEM], 2 * cells * ext * slots * (slots + 2 * ext)
    )(position, cell_ham)

    def block(rows, dtype=F32):
        return ((rows, width), dtype)

    start, p_o, s_o = call(
        first_o_kernel,
        [block(ext, BF16), block(edge), block(edge, BF16)],
        [VMEM] * 5,
        flops(edge, ext),
    )(wavefunctions, halo_e, halo_o, *operator)
    r_o = swap_odd(s_o)
    scale, p_e, y_m, v_m = call(
        first_e_kernel,
        [block(ext), block(edge), block(inner), block(inner, BF16)],
        [VMEM] * 6,
        flops(ext - edge, ext),
    )(start, halo_e, halo_o, masses, *operator)
    s_e = p_e
    y_e = y_o = start
    w_m = start
    w_e = w_o = None
    for step in range(1, DEGREE):
        last = step == DEGREE - 1
        r_e = swap_even(s_e)
        (part,) = call(
            functools.partial(middle_kernel, edge), [block(ext)], [VMEM] * 3, flops(ext, inner)
        )(v_m, *operator)
        first = step == 1
        new_e, part_o, part_e = call(
            even_first_kernel if first else even_kernel,
            [block(edge), block(edge), block(ext - edge)],
            [VMEM] * (7 if first else 8),
            flops(ext, edge),
        )(r_e, p_e, scale, y_e, *(() if first else (w_e,)), part, *operator)
        new_o, v_o, p_o, s_o = call(
            functools.partial(odd_kernel, first, last),
            [block(edge), block(edge, BF16), block(edge), block(g if last else edge, BF16)],
            [VMEM] * (7 if first else 8),
            flops(edge, edge),
        )(r_o, p_o, scale, y_o, *(() if first else (w_o,)), part_o, *operator)
        r_o = swap_odd(s_o)
        outs = call(
            functools.partial(rest_kernel, last),
            [block(edge)] + ([block(inner, BF16), block(g)] if last else [block(inner), block(inner, BF16)]),
            [VMEM] * 7,
            flops(ext - edge, edge),
        )(v_o, part_e, scale, y_m, w_m, *operator)
        w_e = start[ext - edge :].astype(F32) if first else y_e
        w_o = start[:edge].astype(F32) if first else y_o
        y_e, y_o, w_m = new_e, new_o, y_m
        if last:
            p_e, f_m, s_e = outs
        else:
            p_e, y_m, v_m = outs
            s_e = p_e
    r_e = swap_even(s_e)
    far_m = spread(f_m)
    (f_b,) = call(
        last_kernel, [block(edge, BF16)], [VMEM] * 9, edge * width * 8
    )(r_e, r_o, p_e, p_o, scale, y_e, y_o, w_e, w_o)
    far_b = spread(f_b)
    (filtered,) = call(join_kernel, [block(owned, BF16)], [VMEM] * 2, 1 << 10)(
        f_m, f_b
    )
    total = bands * width
    (before,) = call(
        functools.partial(margin_kernel, bands, True),
        [((total, width), F32)],
        [VMEM] * bands,
        2 * total * width * inner,
    )(f_m, *far_m)
    (sums,) = call(
        functools.partial(margin_kernel, bands, False),
        [((total, width), BF16)],
        [VMEM] * (bands + 1),
        2 * total * width * edge,
    )(before, f_b, *far_b)
    parts = lax.all_to_all(sums.reshape(domains, total // domains, width), "dom", 0, 0)
    factor = 1.0 / jnp.sqrt(F32(owned * domains))
    return (filtered, (jnp.sum(parts.astype(F32), axis=0) * factor).T)


def solution(mesh):
    return jax.shard_map(
        shards,
        mesh=mesh,
        in_specs=(P("dom", "band"), P("dom", None, None), P("dom", None), P("dom"), P("dom")),
        out_specs=(P("dom", "band"), P("band", "dom")),
        check_vma=False,
    )
```

```python
import functools

import jax
import jax.numpy as jnp
from jax import lax
from jax.experimental import pallas as pl
from jax.experimental.pallas import tpu as pltpu
from jax.sharding import PartitionSpec as P


DEGREE = 4
LANES = 128
PAD = 16
VMEM_LIMIT = 16 << 20

filter_center = 0.5
filter_halfwidth = 3.0

F32 = jnp.float32
BF16 = jnp.bfloat16
VMEM = pl.BlockSpec(memory_space=pltpu.VMEM)
SMEM = pl.BlockSpec(memory_space=pltpu.SMEM)
HBM = pl.BlockSpec(memory_space=pltpu.HBM)


def call(kernel, outs, ins, flops, scratch=()):
    return pl.pallas_call(
        kernel,
        out_shape=[jax.ShapeDtypeStruct(s, d) for s, d in outs],
        in_specs=ins,
        out_specs=[VMEM] * len(outs),
        scratch_shapes=list(scratch),
        cost_estimate=pl.CostEstimate(flops=flops, bytes_accessed=1 << 20, transcendentals=0),
        compiler_params=pltpu.CompilerParams(vmem_limit_bytes=VMEM_LIMIT),
    )


def is_odd():
    return jnp.bitwise_and(lax.axis_index("dom"), 1) == 1


def at(start, size):
    return pl.ds(pl.multiple_of(start, LANES), size)


def to_columns(row):
    width = row.shape[1]
    parts = [
        jnp.broadcast_to(row[:, i : i + LANES], (LANES, LANES)).T for i in range(0, width, LANES)
    ]
    return parts[0] if len(parts) == 1 else jnp.concatenate(parts, axis=0)


def split(x):
    high = x.astype(BF16)
    return high, (x - high.astype(F32)).astype(BF16)


def dot(a, b):
    return jnp.dot(a, b, preferred_element_type=F32)


def apply(hi_ref, lo_ref, cols, values):
    return dot(hi_ref[:, cols], values) + dot(lo_ref[:, cols], values)


def advance(applied, current, previous):
    moved = (applied - filter_center * current) / filter_halfwidth
    return moved if previous is None else 2.0 * moved - previous


def rim_kernel(
    count_ref, v_hbm, d_hbm, conn_hbm, ham_hbm, ro_ref, re_ref, v_ref, d_ref, pos_ref, ham_ref, sems
):
    pairs = (
        (ham_hbm, ham_ref),
        (v_hbm, v_ref),
        (d_hbm, d_ref),
        (conn_hbm, pos_ref),
    )
    copies = [pltpu.make_async_copy(a, b, sems.at[i]) for i, (a, b) in enumerate(pairs)]
    for copy in copies[1:] + copies[:1]:
        copy.start()
    odd = is_odd()
    owned = v_ref.shape[0]
    g = ro_ref.shape[0] - PAD
    far = owned - g
    row = lax.broadcasted_iota(jnp.int32, (PAD, LANES), 0)
    for copy in copies[1:]:
        copy.wait()
    for out, edge in ((ro_ref, jnp.where(odd, far, 0)), (re_ref, jnp.where(odd, 0, far))):
        out[:g, :] = v_ref[at(edge, g), :]
        mass = d_ref[pl.ds(edge // LANES, 1), :]
        high = mass.astype(BF16).astype(F32)
        out[g:, :] = jnp.where(row == 0, high, jnp.where(row == 1, mass - high, 0.0)).astype(BF16)
    cells, slots = pos_ref.shape
    edge = slots // 2
    base = owned + 2 * g - edge
    conn = pos_ref[...]
    turned = jnp.where(conn < edge, conn + base, jnp.where(conn >= base, conn - base, conn))
    live = lax.broadcasted_iota(jnp.int32, (cells, slots), 0) < count_ref[0]
    pos_ref[...] = jnp.where(live, jnp.where(odd, turned, conn), -1)
    copies[0].wait()


def gather_rows(pos_ref, ham_ref, pick_ref, first, count):
    cells, slots = pos_ref.shape
    total = None
    for c in range(cells):
        row = pos_ref[c : c + 1, :]
        spread = lax.broadcasted_iota(jnp.int32, (count, slots), 0) + first == row
        spread = jnp.where(spread, 1.0, 0.0).astype(BF16)
        high, low = split(dot(spread, ham_ref[c]))
        pick = pick_ref[c * slots : (c + 1) * slots, :]
        part = dot(high, pick) + dot(low, pick)
        total = part if total is None else total + part
    return split(total)


def assemble_o_kernel(pos_ref, ham_ref, hi_ref, lo_ref, pick_ref, corner_ref):
    edge, ext = hi_ref.shape
    cells, slots = pos_ref.shape
    lane = lax.broadcasted_iota(jnp.int32, (slots, LANES), 1)
    for c in range(cells):
        column = to_columns(pos_ref[c : c + 1, :].astype(F32)).astype(jnp.int32)
        for i in range(0, ext, LANES):
            pick_ref[c * slots : (c + 1) * slots, i : i + LANES] = jnp.where(
                lane + i == column, 1.0, 0.0
            ).astype(BF16)
    high, low = gather_rows(pos_ref, ham_ref, pick_ref, 0, edge)
    hi_ref[...] = high
    lo_ref[...] = low
    corner_ref[:, :edge] = high[:, :edge]
    corner_ref[:, edge:] = low[:, :edge]


def assemble_r_kernel(pos_ref, ham_ref, pick_ref, hi_ref, lo_ref):
    rest, ext = hi_ref.shape
    hi_ref[...], lo_ref[...] = gather_rows(pos_ref, ham_ref, pick_ref, ext - rest, rest)


def first_o_kernel(v_ref, he_ref, ho_ref, hi_ref, lo_ref, vx_ref, p_ref, s_ref):
    odd = is_odd()
    owned = v_ref.shape[0]
    ext = hi_ref.shape[1]
    g = (ext - owned) // 2
    base = ext - 2 * g
    far = owned - g
    vx_ref[at(jnp.where(odd, g, 0), g), :] = ho_ref[:g, :]
    vx_ref[at(jnp.where(odd, 0, g), g), :] = v_ref[at(jnp.where(odd, far, 0), g), :]
    vx_ref[2 * g : base, :] = v_ref[g:far, :]
    vx_ref[at(base + jnp.where(odd, 0, g), g), :] = he_ref[:g, :]
    vx_ref[at(base + jnp.where(odd, g, 0), g), :] = v_ref[at(jnp.where(odd, 0, far), g), :]
    product = apply(hi_ref, lo_ref, slice(None), vx_ref[...])
    p_ref[...] = product
    s_ref[...] = product.astype(BF16)


def first_e_kernel(vx_ref, he_ref, ho_ref, d_ref, hi_ref, lo_ref, c_ref, p_ref, y_ref, v_ref):
    odd = is_odd()
    ext = hi_ref.shape[1]
    g = he_ref.shape[0] - PAD
    owned = ext - 2 * g
    base = ext - 2 * g
    far = owned - g

    def mass(ref):
        return to_columns(jnp.sum(ref[g:, :].astype(F32), axis=0, keepdims=True))

    def own(block):
        return to_columns(d_ref[pl.ds(block, 1), :])

    c_ref[at(jnp.where(odd, g, 0), g), :] = mass(ho_ref)
    c_ref[at(jnp.where(odd, 0, g), g), :] = own(jnp.where(odd, far // LANES, 0))
    for i in range(1, far // LANES):
        c_ref[g + i * LANES : g + (i + 1) * LANES, :] = own(i)
    c_ref[at(base + jnp.where(odd, 0, g), g), :] = mass(he_ref)
    c_ref[at(base + jnp.where(odd, g, 0), g), :] = own(jnp.where(odd, 0, far // LANES))
    product = apply(hi_ref, lo_ref, slice(None), vx_ref[...])
    p_ref[...] = product[base - 2 * g :]
    middle = slice(2 * g, base)
    y = advance(c_ref[middle, :] * product[: base - 2 * g], vx_ref[middle, :].astype(F32), None)
    y_ref[...] = y
    v_ref[...] = y.astype(BF16)


def middle_kernel(v_ref, ho_ref, lo_ref, hr_ref, lr_ref, po_ref, pr_ref):
    edge = ho_ref.shape[0]
    inner = slice(edge, edge + v_ref.shape[0])
    po_ref[...] = apply(ho_ref, lo_ref, inner, v_ref[...])
    pr_ref[...] = apply(hr_ref, lr_ref, inner, v_ref[...])


def even_kernel(
    first, last, r_ref, p_ref, c_ref, y_ref, *rest
):
    rest = list(rest)
    prev_ref = None if first else rest.pop(0)
    mo_ref, mr_ref, ho_ref, lo_ref, hr_ref, lr_ref, y_out, po_out, pr_out, s_out = rest
    ext = ho_ref.shape[1]
    edge = r_ref.shape[0]
    block = slice(ext - edge, ext)
    current = y_ref[block, :].astype(F32) if first else y_ref[...]
    previous = None if first else tail(prev_ref, edge)
    y = advance(c_ref[block, :] * (p_ref[...] + r_ref[...]), current, previous)
    y_out[...] = y
    values = y.astype(BF16)
    part = mo_ref[...] + apply(ho_ref, lo_ref, block, values)
    po_out[...] = part
    if last:
        g = s_out.shape[0]
        s_out[...] = po_out[at(jnp.where(is_odd(), g, 0), g), :].astype(BF16)
    else:
        s_out[...] = part.astype(BF16)
    pr_out[...] = mr_ref[...] + apply(hr_ref, lr_ref, block, values)


def tail(ref, size):
    return ref[ref.shape[0] - size :, :].astype(F32)


def head(ref, size):
    return ref[:size, :].astype(F32)


def corner(ho_ref, lo_ref, k_ref, values):
    edge = values.shape[0]
    return (
        apply(ho_ref, lo_ref, slice(0, edge), values)
        + dot(k_ref[:, :edge], values)
        + dot(k_ref[:, edge:], values)
    )


def odd_first_kernel(r_ref, p_ref, c_ref, y_ref, y_out, v_out):
    edge = r_ref.shape[0]
    y = advance(c_ref[:edge, :] * (p_ref[...] + r_ref[...].astype(F32)), head(y_ref, edge), None)
    y_out[...] = y
    v_out[...] = y.astype(BF16)


def odd_kernel(r_ref, p_ref, v_ref, c_ref, y_ref, prev_ref, ho_ref, lo_ref, k_ref, y_out, v_out):
    edge = r_ref.shape[0]
    total = p_ref[...] + r_ref[...].astype(F32) + corner(ho_ref, lo_ref, k_ref, v_ref[...])
    y = advance(c_ref[:edge, :] * total, head(y_ref, edge), head(prev_ref, edge))
    y_out[...] = y
    v_out[...] = y.astype(BF16)


def rest_kernel(last, v_ref, part_ref, c_ref, y_ref, prev_ref, hr_ref, lr_ref, p_out, *outs):
    ext = hr_ref.shape[1]
    edge = v_ref.shape[0]
    base = ext - edge
    product = part_ref[...] + apply(hr_ref, lr_ref, slice(0, edge), v_ref[...])
    p_out[...] = product[base - edge :]
    middle = slice(edge, base)
    y = advance(
        c_ref[middle, :] * product[: base - edge],
        y_ref[...],
        prev_ref[middle, :].astype(F32) if prev_ref.shape[0] == ext else prev_ref[...],
    )
    if last:
        f_out, s_out = outs
        f_out[...] = y.astype(BF16)
        g = s_out.shape[0]
        s_out[...] = p_out[at(jnp.where(is_odd(), 0, g), g), :]
    else:
        y_out, v_out = outs
        y_out[...] = y
        v_out[...] = y.astype(BF16)


def corner_kernel(v_ref, p_ref, ho_ref, lo_ref, k_ref, p_out):
    p_out[...] = p_ref[...] + corner(ho_ref, lo_ref, k_ref, v_ref[...])


def last_kernel(re_ref, ro_ref, pe_ref, po_ref, c_ref, ye_ref, yo_ref, we_ref, wo_ref, f_ref):
    odd = is_odd()
    ext = c_ref.shape[0]
    g = re_ref.shape[0]
    base = ext - 2 * g
    here = at(jnp.where(odd, 0, g), g)
    total = po_ref[here, :] + ro_ref[...].astype(F32)
    f_ref[:g, :] = advance(c_ref[here, :] * total, yo_ref[here, :], wo_ref[here, :]).astype(BF16)
    here = at(jnp.where(odd, g, 0), g)
    total = pe_ref[here, :] + re_ref[...]
    scale = c_ref[at(base + jnp.where(odd, g, 0), g), :]
    f_ref[g:, :] = advance(scale * total, ye_ref[here, :], we_ref[here, :]).astype(BF16)


def join_kernel(fm_ref, fb_ref, out_ref):
    odd = is_odd()
    g = fb_ref.shape[0] // 2
    far = out_ref.shape[0] - g
    out_ref[g:far, :] = fm_ref[...]
    out_ref[at(jnp.where(odd, far, 0), g), :] = fb_ref[:g, :]
    out_ref[at(jnp.where(odd, 0, far), g), :] = fb_ref[g:, :]


def margin_kernel(bands, start, *refs):
    refs = list(refs)
    before = None if start else refs.pop(0)
    out_ref = refs.pop()
    own = refs[0][...]
    width = own.shape[1]
    for k in range(bands):
        other = own if k == 0 else refs[k][...]
        block = lax.dot_general(other, own, (((0,), (0,)), ((), ())), preferred_element_type=F32)
        place = at((lax.axis_index("band") ^ k) * width, width)
        if start:
            out_ref[place, :] = block
        else:
            out_ref[place, :] = (before[place, :] + block).astype(BF16)


def shards(wavefunctions, cell_ham, connectivity, inv_mass, cell_count):
    owned, width = wavefunctions.shape
    cells, slots = connectivity.shape
    g = cell_ham.shape[1] // 4
    edge = 2 * g
    ext = owned + edge
    inner = ext - 2 * edge
    domains = lax.axis_size("dom")
    bands = lax.axis_size("band")
    if domains % 2 or bands & (bands - 1) or g != LANES or width != LANES or slots != 2 * edge:
        raise ValueError("unsupported sizes")
    even_pairs = [(i, i ^ 1) for i in range(domains)]
    odd_pairs = [(i, (i + 1) % domains if i % 2 else (i - 1) % domains) for i in range(domains)]

    def swap_even(x):
        return lax.ppermute(x, "dom", even_pairs)

    def swap_odd(x):
        return lax.ppermute(x, "dom", odd_pairs)

    def spread(x):
        out = []
        for k in range(1, bands):
            out.append(lax.ppermute(x, "band", [(i, i ^ k) for i in range(bands)]))
        return out

    def flops(rows, cols):
        return 4 * rows * cols * width

    masses = inv_mass.reshape(owned // LANES, LANES)
    rim = ((g + PAD, width), BF16)
    inputs = (wavefunctions, masses, connectivity, cell_ham)
    rim_o, rim_e, wavefunctions, masses, position, cell_ham = call(
        rim_kernel,
        [rim, rim] + [(x.shape, x.dtype) for x in inputs],
        [SMEM] + [HBM] * 4,
        1 << 10,
        [pltpu.SemaphoreType.DMA((4,))],
    )(cell_count, *[pltpu.with_memory_space_constraint(x, pltpu.HBM) for x in inputs])
    halo_o = swap_odd(rim_o)
    halo_e = swap_even(rim_e)

    def block(rows, dtype=F32, cols=width):
        return ((rows, cols), dtype)

    *rows_o, pick, corner_mine = call(
        assemble_o_kernel,
        [block(edge, BF16, ext)] * 2 + [block(cells * slots, BF16, ext), block(edge, BF16, 2 * edge)],
        [VMEM] * 2,
        2 * cells * edge * slots * (slots + 2 * ext),
    )(position, cell_ham)
    corner_far = lax.ppermute(corner_mine, "dom", odd_pairs)
    rows_r = call(
        assemble_r_kernel,
        [block(ext - edge, BF16, ext)] * 2,
        [VMEM] * 3,
        2 * cells * (ext - edge) * slots * (slots + 2 * ext),
    )(position, cell_ham, pick)
    rows = (*rows_o, *rows_r)

    start, p_o, s_o = call(
        first_o_kernel,
        [block(ext, BF16), block(edge), block(edge, BF16)],
        [VMEM] * 5,
        flops(edge, ext),
    )(wavefunctions, halo_e, halo_o, *rows_o)
    r_o = swap_odd(s_o)
    scale, p_e, y_m, v_m = call(
        first_e_kernel,
        [block(ext), block(edge), block(inner), block(inner, BF16)],
        [VMEM] * 6,
        flops(ext - edge, ext),
    )(start, halo_e, halo_o, masses, *rows_r)
    s_e = p_e
    y_e = y_o = w_m = start
    w_e = w_o = v_o = None
    for step in range(1, DEGREE):
        last = step == DEGREE - 1
        first = step == 1
        r_e = swap_even(s_e)
        middle = call(
            middle_kernel, [block(edge), block(ext - edge)], [VMEM] * 5, flops(ext, inner)
        )(v_m, *rows)
        new_e, part_o, part_r, s_o = call(
            functools.partial(even_kernel, first, last),
            [block(edge), block(edge), block(ext - edge), block(g if last else edge, BF16)],
            [VMEM] * (10 if first else 11),
            flops(ext, edge),
        )(r_e, p_e, scale, y_e, *(() if first else (w_e,)), *middle, *rows)
        r_next = swap_odd(s_o)
        outs = [block(edge), block(edge, BF16)]
        if first:
            new_o, v_o = call(odd_first_kernel, outs, [VMEM] * 4, 1 << 10)(r_o, p_o, scale, y_o)
        else:
            new_o, v_o = call(odd_kernel, outs, [VMEM] * 9, flops(edge, 2 * edge))(
                r_o, p_o, v_o, scale, y_o, w_o, *rows_o, corner_far
            )
        outs = call(
            functools.partial(rest_kernel, last),
            [block(edge)] + ([block(inner, BF16), block(g)] if last else [block(inner), block(inner, BF16)]),
            [VMEM] * 7,
            flops(ext - edge, edge),
        )(v_o, part_r, scale, y_m, w_m, *rows_r)
        r_o, p_o = r_next, part_o
        w_e, w_o, w_m = y_e, y_o, y_m
        y_e, y_o = new_e, new_o
        if last:
            p_e, f_m, s_e = outs
        else:
            p_e, y_m, v_m = outs
            s_e = p_e
    r_e = swap_even(s_e)
    (p_o,) = call(corner_kernel, [block(edge)], [VMEM] * 5, flops(edge, 2 * edge))(
        v_o, p_o, *rows_o, corner_far
    )
    far_m = spread(f_m)
    (f_b,) = call(
        last_kernel, [block(edge, BF16)], [VMEM] * 9, edge * width * 8
    )(r_e, r_o, p_e, p_o, scale, y_e, y_o, w_e, w_o)
    far_b = spread(f_b)
    (filtered,) = call(join_kernel, [block(owned, BF16)], [VMEM] * 2, 1 << 10)(
        f_m, f_b
    )
    total = bands * width
    (before,) = call(
        functools.partial(margin_kernel, bands, True),
        [((total, width), F32)],
        [VMEM] * bands,
        2 * total * width * inner,
    )(f_m, *far_m)
    (sums,) = call(
        functools.partial(margin_kernel, bands, False),
        [((total, width), BF16)],
        [VMEM] * (bands + 1),
        2 * total * width * edge,
    )(before, f_b, *far_b)
    parts = lax.all_to_all(sums.reshape(domains, total // domains, width), "dom", 0, 0)
    factor = 1.0 / jnp.sqrt(F32(owned * domains))
    return (filtered, (jnp.sum(parts.astype(F32), axis=0) * factor).T)


def solution(mesh):
    return jax.shard_map(
        shards,
        mesh=mesh,
        in_specs=(P("dom", "band"), P("dom", None, None), P("dom", None), P("dom"), P("dom")),
        out_specs=(P("dom", "band"), P("band", "dom")),
        check_vma=False,
    )
```

```python
import functools

import jax
import jax.numpy as jnp
from jax import lax
from jax.experimental import pallas as pl
from jax.experimental.pallas import tpu as pltpu
from jax.sharding import PartitionSpec as P


DEGREE = 4
LANES = 128
PAD = 16
VMEM_LIMIT = 16 << 20

filter_center = 0.5
filter_halfwidth = 3.0

F32 = jnp.float32
BF16 = jnp.bfloat16
VMEM = pl.BlockSpec(memory_space=pltpu.VMEM)
SMEM = pl.BlockSpec(memory_space=pltpu.SMEM)
HBM = pl.BlockSpec(memory_space=pltpu.HBM)


def call(kernel, outs, ins, flops, scratch=()):
    return pl.pallas_call(
        kernel,
        out_shape=[jax.ShapeDtypeStruct(s, d) for s, d in outs],
        in_specs=ins,
        out_specs=[VMEM] * len(outs),
        scratch_shapes=list(scratch),
        cost_estimate=pl.CostEstimate(flops=flops, bytes_accessed=1 << 20, transcendentals=0),
        compiler_params=pltpu.CompilerParams(vmem_limit_bytes=VMEM_LIMIT),
    )


def is_odd():
    return jnp.bitwise_and(lax.axis_index("dom"), 1) == 1


def at(start, size):
    return pl.ds(pl.multiple_of(start, LANES), size)


def to_columns(row):
    width = row.shape[1]
    parts = [
        jnp.broadcast_to(row[:, i : i + LANES], (LANES, LANES)).T for i in range(0, width, LANES)
    ]
    return parts[0] if len(parts) == 1 else jnp.concatenate(parts, axis=0)


def split(x):
    high = x.astype(BF16)
    return high, (x - high.astype(F32)).astype(BF16)


def dot(a, b):
    return jnp.dot(a, b, preferred_element_type=F32)


def apply(hi_ref, lo_ref, cols, values):
    return dot(hi_ref[:, cols], values) + dot(lo_ref[:, cols], values)


def advance(applied, current, previous):
    moved = (applied - filter_center * current) / filter_halfwidth
    return moved if previous is None else 2.0 * moved - previous


def rim_kernel(
    count_ref, v_hbm, d_hbm, conn_hbm, ham_hbm, ro_ref, re_ref, v_ref, d_ref, pos_ref, ham_ref, sems
):
    pairs = (
        (ham_hbm, ham_ref),
        (v_hbm, v_ref),
        (d_hbm, d_ref),
        (conn_hbm, pos_ref),
    )
    copies = [pltpu.make_async_copy(a, b, sems.at[i]) for i, (a, b) in enumerate(pairs)]
    for copy in copies[1:] + copies[:1]:
        copy.start()
    odd = is_odd()
    owned = v_ref.shape[0]
    g = ro_ref.shape[0] - PAD
    far = owned - g
    row = lax.broadcasted_iota(jnp.int32, (PAD, LANES), 0)
    for copy in copies[1:]:
        copy.wait()
    for out, edge in ((ro_ref, jnp.where(odd, far, 0)), (re_ref, jnp.where(odd, 0, far))):
        out[:g, :] = v_ref[at(edge, g), :]
        mass = d_ref[pl.ds(edge // LANES, 1), :]
        high = mass.astype(BF16).astype(F32)
        out[g:, :] = jnp.where(row == 0, high, jnp.where(row == 1, mass - high, 0.0)).astype(BF16)
    cells, slots = pos_ref.shape
    edge = slots // 2
    base = owned + 2 * g - edge
    conn = pos_ref[...]
    turned = jnp.where(conn < edge, conn + base, jnp.where(conn >= base, conn - base, conn))
    live = lax.broadcasted_iota(jnp.int32, (cells, slots), 0) < count_ref[0]
    pos_ref[...] = jnp.where(live, jnp.where(odd, turned, conn), -1)
    copies[0].wait()


def gather_rows(pos_ref, ham_ref, pick_ref, first, count):
    cells, slots = pos_ref.shape
    total = None
    for c in range(cells):
        row = pos_ref[c : c + 1, :]
        spread = lax.broadcasted_iota(jnp.int32, (count, slots), 0) + first == row
        spread = jnp.where(spread, 1.0, 0.0).astype(BF16)
        high, low = split(dot(spread, ham_ref[c]))
        pick = pick_ref[c * slots : (c + 1) * slots, :]
        part = dot(high, pick) + dot(low, pick)
        total = part if total is None else total + part
    return split(total)


def assemble_o_kernel(pos_ref, ham_ref, hi_ref, lo_ref, pick_ref, corner_ref):
    edge, ext = hi_ref.shape
    cells, slots = pos_ref.shape
    lane = lax.broadcasted_iota(jnp.int32, (slots, LANES), 1)
    for c in range(cells):
        column = to_columns(pos_ref[c : c + 1, :].astype(F32)).astype(jnp.int32)
        for i in range(0, ext, LANES):
            pick_ref[c * slots : (c + 1) * slots, i : i + LANES] = jnp.where(
                lane + i == column, 1.0, 0.0
            ).astype(BF16)
    high, low = gather_rows(pos_ref, ham_ref, pick_ref, 0, edge)
    hi_ref[...] = high
    lo_ref[...] = low
    corner_ref[:, :edge] = high[:, :edge]
    corner_ref[:, edge:] = low[:, :edge]


def assemble_r_kernel(pos_ref, ham_ref, pick_ref, hi_ref, lo_ref):
    rest, ext = hi_ref.shape
    hi_ref[...], lo_ref[...] = gather_rows(pos_ref, ham_ref, pick_ref, ext - rest, rest)


def first_o_kernel(v_ref, he_ref, ho_ref, hi_ref, lo_ref, vx_ref, p_ref, s_ref):
    odd = is_odd()
    owned = v_ref.shape[0]
    ext = hi_ref.shape[1]
    g = (ext - owned) // 2
    base = ext - 2 * g
    far = owned - g
    vx_ref[at(jnp.where(odd, g, 0), g), :] = ho_ref[:g, :]
    vx_ref[at(jnp.where(odd, 0, g), g), :] = v_ref[at(jnp.where(odd, far, 0), g), :]
    vx_ref[2 * g : base, :] = v_ref[g:far, :]
    vx_ref[at(base + jnp.where(odd, 0, g), g), :] = he_ref[:g, :]
    vx_ref[at(base + jnp.where(odd, g, 0), g), :] = v_ref[at(jnp.where(odd, 0, far), g), :]
    product = apply(hi_ref, lo_ref, slice(None), vx_ref[...])
    p_ref[...] = product
    s_ref[...] = product.astype(BF16)


def first_e_kernel(vx_ref, hi_ref, lo_ref, p_ref):
    edge = p_ref.shape[0]
    rest = hi_ref.shape[0]
    values = vx_ref[...]
    p_ref[...] = dot(hi_ref[rest - edge :, :], values) + dot(lo_ref[rest - edge :, :], values)


def inner_columns(v, rows, mo_out, mr_out):
    ho_ref, lo_ref, hr_ref, lr_ref = rows
    edge = ho_ref.shape[0]
    inner = slice(edge, edge + v.shape[0])
    mo_out[...] = apply(ho_ref, lo_ref, inner, v)
    mr_out[...] = apply(hr_ref, lr_ref, inner, v)


def first_m_kernel(vx_ref, he_ref, ho_ref, d_ref, *refs):
    rows, (c_ref, y_out, mo_out, mr_out) = refs[:4], refs[4:]
    hr_ref, lr_ref = rows[2:]
    odd = is_odd()
    ext = hr_ref.shape[1]
    g = he_ref.shape[0] - PAD
    owned = ext - 2 * g
    base = ext - 2 * g
    far = owned - g

    def mass(ref):
        return to_columns(jnp.sum(ref[g:, :].astype(F32), axis=0, keepdims=True))

    def own(block):
        return to_columns(d_ref[pl.ds(block, 1), :])

    c_ref[at(jnp.where(odd, g, 0), g), :] = mass(ho_ref)
    c_ref[at(jnp.where(odd, 0, g), g), :] = own(jnp.where(odd, far // LANES, 0))
    for i in range(1, far // LANES):
        c_ref[g + i * LANES : g + (i + 1) * LANES, :] = own(i)
    c_ref[at(base + jnp.where(odd, 0, g), g), :] = mass(he_ref)
    c_ref[at(base + jnp.where(odd, g, 0), g), :] = own(jnp.where(odd, 0, far // LANES))
    middle = slice(2 * g, base)
    inner = base - 2 * g
    values = vx_ref[...]
    product = dot(hr_ref[:inner, :], values) + dot(lr_ref[:inner, :], values)
    y = advance(c_ref[middle, :] * product, vx_ref[middle, :].astype(F32), None)
    y_out[...] = y
    inner_columns(y.astype(BF16), rows, mo_out, mr_out)


def even_kernel(
    first, last, r_ref, p_ref, c_ref, y_ref, *rest
):
    rest = list(rest)
    prev_ref = None if first else rest.pop(0)
    mo_ref, mr_ref, ho_ref, lo_ref, hr_ref, lr_ref, y_out, po_out, pr_out, s_out = rest
    ext = ho_ref.shape[1]
    edge = r_ref.shape[0]
    block = slice(ext - edge, ext)
    current = y_ref[block, :].astype(F32) if first else y_ref[...]
    previous = None if first else tail(prev_ref, edge)
    y = advance(c_ref[block, :] * (p_ref[...] + r_ref[...]), current, previous)
    y_out[...] = y
    values = y.astype(BF16)
    part = mo_ref[...] + apply(ho_ref, lo_ref, block, values)
    po_out[...] = part
    if last:
        g = s_out.shape[0]
        s_out[...] = po_out[at(jnp.where(is_odd(), g, 0), g), :].astype(BF16)
    else:
        s_out[...] = part.astype(BF16)
    pr_out[...] = mr_ref[...] + apply(hr_ref, lr_ref, block, values)


def tail(ref, size):
    return ref[ref.shape[0] - size :, :].astype(F32)


def head(ref, size):
    return ref[:size, :].astype(F32)


def corner(ho_ref, lo_ref, k_ref, values):
    edge = values.shape[0]
    return (
        apply(ho_ref, lo_ref, slice(0, edge), values)
        + dot(k_ref[:, :edge], values)
        + dot(k_ref[:, edge:], values)
    )


def odd_kernel(first, r_ref, p_ref, c_ref, y_ref, *rest):
    y_out, v_out = rest[-2:]
    edge = r_ref.shape[0]
    total = p_ref[...] + r_ref[...].astype(F32)
    previous = None if first else head(rest[0], edge)
    y = advance(c_ref[:edge, :] * total, head(y_ref, edge), previous)
    y_out[...] = y
    v_out[...] = y.astype(BF16)


def rest_e_kernel(v_ref, part_ref, hr_ref, lr_ref, p_out, *s_out):
    edge = v_ref.shape[0]
    rows = slice(hr_ref.shape[0] - edge, hr_ref.shape[0])
    values = v_ref[...]
    p_out[...] = (
        part_ref[rows, :]
        + dot(hr_ref[rows, :edge], values)
        + dot(lr_ref[rows, :edge], values)
    )
    if s_out:
        g = s_out[0].shape[0]
        s_out[0][...] = p_out[at(jnp.where(is_odd(), 0, g), g), :]


def next_inner(v_ref, part_ref, c_ref, y_ref, prev_ref, hr_ref, lr_ref):
    ext = hr_ref.shape[1]
    edge = v_ref.shape[0]
    inner = y_ref.shape[0]
    values = v_ref[...]
    product = (
        part_ref[:inner, :] + dot(hr_ref[:inner, :edge], values) + dot(lr_ref[:inner, :edge], values)
    )
    middle = slice(edge, edge + inner)
    previous = prev_ref[middle, :].astype(F32) if prev_ref.shape[0] == ext else prev_ref[...]
    return advance(c_ref[middle, :] * product, y_ref[...], previous)


def rest_m_kernel(v_ref, part_ref, po_ref, c_ref, y_ref, prev_ref, k_ref, *refs):
    rows, (y_out, mo_out, mr_out, p_out) = refs[:4], refs[4:]
    y = next_inner(v_ref, part_ref, c_ref, y_ref, prev_ref, *rows[2:])
    y_out[...] = y
    inner_columns(y.astype(BF16), rows, mo_out, mr_out)
    p_out[...] = po_ref[...] + corner(rows[0], rows[1], k_ref, v_ref[...])


def last_m_kernel(v_ref, part_ref, c_ref, y_ref, prev_ref, hr_ref, lr_ref, f_out):
    f_out[...] = next_inner(v_ref, part_ref, c_ref, y_ref, prev_ref, hr_ref, lr_ref).astype(BF16)


def corner_kernel(v_ref, p_ref, ho_ref, lo_ref, k_ref, p_out):
    p_out[...] = p_ref[...] + corner(ho_ref, lo_ref, k_ref, v_ref[...])


def last_kernel(re_ref, ro_ref, pe_ref, po_ref, c_ref, ye_ref, yo_ref, we_ref, wo_ref, fm_ref, f_ref, all_ref):
    odd = is_odd()
    ext = c_ref.shape[0]
    g = re_ref.shape[0]
    base = ext - 2 * g
    here = at(jnp.where(odd, 0, g), g)
    total = po_ref[here, :] + ro_ref[...].astype(F32)
    f_ref[:g, :] = advance(c_ref[here, :] * total, yo_ref[here, :], wo_ref[here, :]).astype(BF16)
    here = at(jnp.where(odd, g, 0), g)
    total = pe_ref[here, :] + re_ref[...]
    scale = c_ref[at(base + jnp.where(odd, g, 0), g), :]
    f_ref[g:, :] = advance(scale * total, ye_ref[here, :], we_ref[here, :]).astype(BF16)
    inner = fm_ref.shape[0]
    all_ref[:inner, :] = fm_ref[...]
    all_ref[inner:, :] = f_ref[...]


def join_kernel(all_ref, out_ref):
    odd = is_odd()
    g = LANES
    far = out_ref.shape[0] - g
    inner = far - g
    out_ref[g:far, :] = all_ref[:inner, :]
    out_ref[at(jnp.where(odd, far, 0), g), :] = all_ref[inner : inner + g, :]
    out_ref[at(jnp.where(odd, 0, far), g), :] = all_ref[inner + g :, :]


def gram(a, b):
    return lax.dot_general(a, b, (((0,), (0,)), ((), ())), preferred_element_type=F32)


def place(k, width):
    return at((lax.axis_index("band") ^ k) * width, width)


def margin_m_kernel(own_ref, *refs):
    out_ref = refs[-1]
    width = own_ref.shape[1]
    for i, ref in enumerate(refs[:-1]):
        out_ref[i * width : (i + 1) * width, :] = gram(ref[...], own_ref[...])


def margin_b_kernel(all_ref, near_ref, before_ref, own_ref, *refs):
    out_ref = refs[-1]
    width = own_ref.shape[1]
    out_ref[place(0, width), :] = gram(all_ref[...], all_ref[...]).astype(BF16)
    out_ref[place(1, width), :] = gram(near_ref[...], all_ref[...]).astype(BF16)
    for i, ref in enumerate(refs[:-1]):
        block = before_ref[i * width : (i + 1) * width, :] + gram(ref[...], own_ref[...])
        out_ref[place(i + 2, width), :] = block.astype(BF16)


def shards(wavefunctions, cell_ham, connectivity, inv_mass, cell_count):
    owned, width = wavefunctions.shape
    cells, slots = connectivity.shape
    g = cell_ham.shape[1] // 4
    edge = 2 * g
    ext = owned + edge
    inner = ext - 2 * edge
    domains = lax.axis_size("dom")
    bands = lax.axis_size("band")
    if domains % 2 or bands & (bands - 1) or g != LANES or width != LANES or slots != 2 * edge:
        raise ValueError("unsupported sizes")
    even_pairs = [(i, i ^ 1) for i in range(domains)]
    odd_pairs = [(i, (i + 1) % domains if i % 2 else (i - 1) % domains) for i in range(domains)]

    def swap_even(x):
        return lax.ppermute(x, "dom", even_pairs)

    def swap_odd(x):
        return lax.ppermute(x, "dom", odd_pairs)

    def shift(x, k):
        return lax.ppermute(x, "band", [(i, i ^ k) for i in range(bands)])

    def flops(rows, cols):
        return 4 * rows * cols * width

    masses = inv_mass.reshape(owned // LANES, LANES)
    rim = ((g + PAD, width), BF16)
    inputs = (wavefunctions, masses, connectivity, cell_ham)
    rim_o, rim_e, wavefunctions, masses, position, cell_ham = call(
        rim_kernel,
        [rim, rim] + [(x.shape, x.dtype) for x in inputs],
        [SMEM] + [HBM] * 4,
        1 << 10,
        [pltpu.SemaphoreType.DMA((4,))],
    )(cell_count, *[pltpu.with_memory_space_constraint(x, pltpu.HBM) for x in inputs])
    halo_o = swap_odd(rim_o)
    halo_e = swap_even(rim_e)

    def block(rows, dtype=F32, cols=width):
        return ((rows, cols), dtype)

    *rows_o, pick, corner_mine = call(
        assemble_o_kernel,
        [block(edge, BF16, ext)] * 2 + [block(cells * slots, BF16, ext), block(edge, BF16, 2 * edge)],
        [VMEM] * 2,
        2 * cells * edge * slots * (slots + 2 * ext),
    )(position, cell_ham)
    corner_far = lax.ppermute(corner_mine, "dom", odd_pairs)
    rows_r = call(
        assemble_r_kernel,
        [block(ext - edge, BF16, ext)] * 2,
        [VMEM] * 3,
        2 * cells * (ext - edge) * slots * (slots + 2 * ext),
    )(position, cell_ham, pick)
    rows = (*rows_o, *rows_r)

    start, p_o, s_o = call(
        first_o_kernel,
        [block(ext, BF16), block(edge), block(edge, BF16)],
        [VMEM] * 5,
        flops(edge, ext),
    )(wavefunctions, halo_e, halo_o, *rows_o)
    r_o = swap_odd(s_o)
    (p_e,) = call(first_e_kernel, [block(edge)], [VMEM] * 3, flops(edge, ext))(start, *rows_r)
    s_e = p_e
    parts_m = [block(edge), block(ext - edge)]
    y_e = y_o = w_m = start
    w_e = w_o = v_o = y_m = part_o = part_r = None
    for step in range(1, DEGREE):
        last = step == DEGREE - 1
        first = step == 1
        r_e = swap_even(s_e)
        if first:
            scale, y_m, *middle = call(
                first_m_kernel, [block(ext), block(inner)] + parts_m, [VMEM] * 8, flops(ext, ext)
            )(start, halo_e, halo_o, masses, *rows)
        else:
            new_m, *middle, p_o = call(
                rest_m_kernel,
                [block(inner)] + parts_m + [block(edge)],
                [VMEM] * 11,
                flops(ext, ext),
            )(v_o, part_r, part_o, scale, y_m, w_m, corner_far, *rows)
            w_m, y_m = y_m, new_m
        new_e, part_o, part_r, s_o = call(
            functools.partial(even_kernel, first, last),
            [block(edge), block(edge), block(ext - edge), block(g if last else edge, BF16)],
            [VMEM] * (10 if first else 11),
            flops(ext, edge),
        )(r_e, p_e, scale, y_e, *(() if first else (w_e,)), *middle, *rows)
        r_next = swap_odd(s_o)
        new_o, v_o = call(
            functools.partial(odd_kernel, first),
            [block(edge), block(edge, BF16)],
            [VMEM] * (4 if first else 5),
            1 << 10,
        )(r_o, p_o, scale, y_o, *(() if first else (w_o,)))
        p_e, *half = call(
            rest_e_kernel, [block(edge)] + [block(g)] * last, [VMEM] * 4, flops(edge, edge)
        )(v_o, part_r, *rows_r)
        s_e = half[0] if last else p_e
        r_o = r_next
        w_e, w_o = y_e, y_o
        y_e, y_o = new_e, new_o
    r_e = swap_even(s_e)
    (f_m,) = call(last_m_kernel, [block(inner, BF16)], [VMEM] * 7, flops(inner, edge))(
        v_o, part_r, scale, y_m, w_m, *rows_r
    )
    far_m = [shift(f_m, k) for k in range(2, bands)]
    (p_o,) = call(corner_kernel, [block(edge)], [VMEM] * 5, flops(edge, 2 * edge))(
        v_o, part_o, *rows_o, corner_far
    )
    f_b, f_all = call(
        last_kernel, [block(edge, BF16), block(owned, BF16)], [VMEM] * 10, edge * width * 8
    )(r_e, r_o, p_e, p_o, scale, y_e, y_o, w_e, w_o, f_m)
    far_b = [shift(f_b, k) for k in range(2, bands)]
    near = shift(f_all, 1)
    (filtered,) = call(join_kernel, [block(owned, BF16)], [VMEM], 1 << 10)(f_all)
    total = bands * width
    (before,) = call(
        margin_m_kernel,
        [((total - 2 * width, width), F32)],
        [VMEM] * (bands - 1),
        2 * total * width * inner,
    )(f_m, *far_m)
    (sums,) = call(
        margin_b_kernel, [((total, width), BF16)], [VMEM] * (bands + 2), 2 * total * width * owned
    )(f_all, near, before, f_b, *far_b)
    parts = lax.all_to_all(sums.reshape(domains, total // domains, width), "dom", 0, 0)
    factor = 1.0 / jnp.sqrt(F32(owned * domains))
    return (filtered, (jnp.sum(parts.astype(F32), axis=0) * factor).T)


def solution(mesh):
    return jax.shard_map(
        shards,
        mesh=mesh,
        in_specs=(P("dom", "band"), P("dom", None, None), P("dom", None), P("dom"), P("dom")),
        out_specs=(P("dom", "band"), P("band", "dom")),
        check_vma=False,
    )
```

```python
import functools

import jax
import jax.numpy as jnp
from jax import lax
from jax.experimental import pallas as pl
from jax.experimental.pallas import tpu as pltpu
from jax.sharding import PartitionSpec as P


DEGREE = 4
LANES = 128
PAD = 16
VMEM_LIMIT = 16 << 20

filter_center = 0.5
filter_halfwidth = 3.0

F32 = jnp.float32
BF16 = jnp.bfloat16
VMEM = pl.BlockSpec(memory_space=pltpu.VMEM)
SMEM = pl.BlockSpec(memory_space=pltpu.SMEM)
HBM = pl.BlockSpec(memory_space=pltpu.HBM)


def call(kernel, outs, ins, flops, scratch=()):
    return pl.pallas_call(
        kernel,
        out_shape=[jax.ShapeDtypeStruct(s, d) for s, d in outs],
        in_specs=ins,
        out_specs=[VMEM] * len(outs),
        scratch_shapes=list(scratch),
        cost_estimate=pl.CostEstimate(flops=flops, bytes_accessed=1 << 20, transcendentals=0),
        compiler_params=pltpu.CompilerParams(vmem_limit_bytes=VMEM_LIMIT),
    )


def is_odd():
    return jnp.bitwise_and(lax.axis_index("dom"), 1) == 1


def at(start, size):
    return pl.ds(pl.multiple_of(start, LANES), size)


def to_columns(row):
    width = row.shape[1]
    parts = [
        jnp.broadcast_to(row[:, i : i + LANES], (LANES, LANES)).T for i in range(0, width, LANES)
    ]
    return parts[0] if len(parts) == 1 else jnp.concatenate(parts, axis=0)


def split(x):
    high = x.astype(BF16)
    return high, (x - high.astype(F32)).astype(BF16)


def dot(a, b):
    return jnp.dot(a, b, preferred_element_type=F32)


def apply(hi_ref, lo_ref, cols, values):
    return dot(hi_ref[:, cols], values) + dot(lo_ref[:, cols], values)


def advance(applied, current, previous):
    moved = (applied - filter_center * current) / filter_halfwidth
    return moved if previous is None else 2.0 * moved - previous


def rim_kernel(
    count_ref, v_hbm, d_hbm, conn_hbm, ham_hbm, ro_ref, re_ref, v_ref, d_ref, pos_ref, ham_ref, sems
):
    pairs = (
        (ham_hbm, ham_ref),
        (v_hbm, v_ref),
        (d_hbm, d_ref),
        (conn_hbm, pos_ref),
    )
    copies = [pltpu.make_async_copy(a, b, sems.at[i]) for i, (a, b) in enumerate(pairs)]
    for copy in copies[1:] + copies[:1]:
        copy.start()
    odd = is_odd()
    owned = v_ref.shape[0]
    g = ro_ref.shape[0] - PAD
    far = owned - g
    row = lax.broadcasted_iota(jnp.int32, (PAD, LANES), 0)
    for copy in copies[1:]:
        copy.wait()
    for out, edge in ((ro_ref, jnp.where(odd, far, 0)), (re_ref, jnp.where(odd, 0, far))):
        out[:g, :] = v_ref[at(edge, g), :]
        mass = d_ref[pl.ds(edge // LANES, 1), :]
        high = mass.astype(BF16).astype(F32)
        out[g:, :] = jnp.where(row == 0, high, jnp.where(row == 1, mass - high, 0.0)).astype(BF16)
    cells, slots = pos_ref.shape
    edge = slots // 2
    base = owned + 2 * g - edge
    conn = pos_ref[...]
    turned = jnp.where(conn < edge, conn + base, jnp.where(conn >= base, conn - base, conn))
    live = lax.broadcasted_iota(jnp.int32, (cells, slots), 0) < count_ref[0]
    pos_ref[...] = jnp.where(live, jnp.where(odd, turned, conn), -1)
    copies[0].wait()


def gather_rows(pos_ref, ham_ref, pick_ref, first, count):
    cells, slots = pos_ref.shape
    total = None
    for c in range(cells):
        row = pos_ref[c : c + 1, :]
        spread = lax.broadcasted_iota(jnp.int32, (count, slots), 0) + first == row
        spread = jnp.where(spread, 1.0, 0.0).astype(BF16)
        high, low = split(dot(spread, ham_ref[c]))
        pick = pick_ref[c * slots : (c + 1) * slots, :]
        part = dot(high, pick) + dot(low, pick)
        total = part if total is None else total + part
    return split(total)


def assemble_o_kernel(pos_ref, ham_ref, hi_ref, lo_ref, pick_ref, corner_ref):
    edge, ext = hi_ref.shape
    cells, slots = pos_ref.shape
    lane = lax.broadcasted_iota(jnp.int32, (slots, LANES), 1)
    for c in range(cells):
        column = to_columns(pos_ref[c : c + 1, :].astype(F32)).astype(jnp.int32)
        for i in range(0, ext, LANES):
            pick_ref[c * slots : (c + 1) * slots, i : i + LANES] = jnp.where(
                lane + i == column, 1.0, 0.0
            ).astype(BF16)
    high, low = gather_rows(pos_ref, ham_ref, pick_ref, 0, edge)
    hi_ref[...] = high
    lo_ref[...] = low
    corner_ref[:, :edge] = high[:, :edge]
    corner_ref[:, edge:] = low[:, :edge]


def assemble_r_kernel(pos_ref, ham_ref, pick_ref, hi_ref, lo_ref):
    rest, ext = hi_ref.shape
    hi_ref[...], lo_ref[...] = gather_rows(pos_ref, ham_ref, pick_ref, ext - rest, rest)


def first_o_kernel(v_ref, he_ref, ho_ref, hi_ref, lo_ref, vx_ref, p_ref, s_ref):
    odd = is_odd()
    owned = v_ref.shape[0]
    ext = hi_ref.shape[1]
    g = (ext - owned) // 2
    base = ext - 2 * g
    far = owned - g
    vx_ref[at(jnp.where(odd, g, 0), g), :] = ho_ref[:g, :]
    vx_ref[at(jnp.where(odd, 0, g), g), :] = v_ref[at(jnp.where(odd, far, 0), g), :]
    vx_ref[2 * g : base, :] = v_ref[g:far, :]
    vx_ref[at(base + jnp.where(odd, 0, g), g), :] = he_ref[:g, :]
    vx_ref[at(base + jnp.where(odd, g, 0), g), :] = v_ref[at(jnp.where(odd, 0, far), g), :]
    product = apply(hi_ref, lo_ref, slice(None), vx_ref[...])
    p_ref[...] = product
    s_ref[...] = product.astype(BF16)


def first_e_kernel(vx_ref, hi_ref, lo_ref, p_ref):
    edge = p_ref.shape[0]
    rest = hi_ref.shape[0]
    values = vx_ref[...]
    p_ref[...] = dot(hi_ref[rest - edge :, :], values) + dot(lo_ref[rest - edge :, :], values)


def inner_columns(v, rows, mo_out, mr_out):
    ho_ref, lo_ref, hr_ref, lr_ref = rows
    edge = ho_ref.shape[0]
    inner = slice(edge, edge + v.shape[0])
    mo_out[...] = apply(ho_ref, lo_ref, inner, v)
    mr_out[...] = apply(hr_ref, lr_ref, inner, v)


def first_m_kernel(vx_ref, he_ref, ho_ref, d_ref, *refs):
    rows, (c_ref, y_out, mo_out, mr_out) = refs[:4], refs[4:]
    hr_ref, lr_ref = rows[2:]
    odd = is_odd()
    ext = hr_ref.shape[1]
    g = he_ref.shape[0] - PAD
    owned = ext - 2 * g
    base = ext - 2 * g
    far = owned - g

    def mass(ref):
        return to_columns(jnp.sum(ref[g:, :].astype(F32), axis=0, keepdims=True))

    def own(block):
        return to_columns(d_ref[pl.ds(block, 1), :])

    c_ref[at(jnp.where(odd, g, 0), g), :] = mass(ho_ref)
    c_ref[at(jnp.where(odd, 0, g), g), :] = own(jnp.where(odd, far // LANES, 0))
    for i in range(1, far // LANES):
        c_ref[g + i * LANES : g + (i + 1) * LANES, :] = own(i)
    c_ref[at(base + jnp.where(odd, 0, g), g), :] = mass(he_ref)
    c_ref[at(base + jnp.where(odd, g, 0), g), :] = own(jnp.where(odd, 0, far // LANES))
    middle = slice(2 * g, base)
    inner = base - 2 * g
    values = vx_ref[...]
    product = dot(hr_ref[:inner, :], values) + dot(lr_ref[:inner, :], values)
    y = advance(c_ref[middle, :] * product, vx_ref[middle, :].astype(F32), None)
    y_out[...] = y
    inner_columns(y.astype(BF16), rows, mo_out, mr_out)


def even_kernel(
    first, last, r_ref, p_ref, c_ref, y_ref, *rest
):
    rest = list(rest)
    prev_ref = None if first else rest.pop(0)
    mo_ref, mr_ref, ho_ref, lo_ref, hr_ref, lr_ref, y_out, po_out, pr_out, s_out = rest
    ext = ho_ref.shape[1]
    edge = r_ref.shape[0]
    block = slice(ext - edge, ext)
    current = y_ref[block, :].astype(F32) if first else y_ref[...]
    previous = None if first else tail(prev_ref, edge)
    y = advance(c_ref[block, :] * (p_ref[...] + r_ref[...]), current, previous)
    y_out[...] = y
    values = y.astype(BF16)
    part = mo_ref[...] + apply(ho_ref, lo_ref, block, values)
    po_out[...] = part
    if last:
        g = s_out.shape[0]
        s_out[...] = po_out[at(jnp.where(is_odd(), g, 0), g), :].astype(BF16)
    else:
        s_out[...] = part.astype(BF16)
    pr_out[...] = mr_ref[...] + apply(hr_ref, lr_ref, block, values)


def tail(ref, size):
    return ref[ref.shape[0] - size :, :].astype(F32)


def head(ref, size):
    return ref[:size, :].astype(F32)


def corner(ho_ref, lo_ref, k_ref, values):
    edge = values.shape[0]
    return (
        apply(ho_ref, lo_ref, slice(0, edge), values)
        + dot(k_ref[:, :edge], values)
        + dot(k_ref[:, edge:], values)
    )


def odd_kernel(first, r_ref, p_ref, c_ref, y_ref, *rest):
    y_out, v_out = rest[-2:]
    edge = r_ref.shape[0]
    total = p_ref[...] + r_ref[...].astype(F32)
    previous = None if first else head(rest[0], edge)
    y = advance(c_ref[:edge, :] * total, head(y_ref, edge), previous)
    y_out[...] = y
    v_out[...] = y.astype(BF16)


def rest_e_kernel(v_ref, part_ref, hr_ref, lr_ref, p_out, *s_out):
    edge = v_ref.shape[0]
    rows = slice(hr_ref.shape[0] - edge, hr_ref.shape[0])
    values = v_ref[...]
    p_out[...] = (
        part_ref[rows, :]
        + dot(hr_ref[rows, :edge], values)
        + dot(lr_ref[rows, :edge], values)
    )
    if s_out:
        g = s_out[0].shape[0]
        s_out[0][...] = p_out[at(jnp.where(is_odd(), 0, g), g), :]


def next_inner(v_ref, part_ref, c_ref, y_ref, prev_ref, hr_ref, lr_ref):
    ext = hr_ref.shape[1]
    edge = v_ref.shape[0]
    inner = y_ref.shape[0]
    values = v_ref[...]
    product = (
        part_ref[:inner, :] + dot(hr_ref[:inner, :edge], values) + dot(lr_ref[:inner, :edge], values)
    )
    middle = slice(edge, edge + inner)
    previous = prev_ref[middle, :].astype(F32) if prev_ref.shape[0] == ext else prev_ref[...]
    return advance(c_ref[middle, :] * product, y_ref[...], previous)


def rest_m_kernel(v_ref, part_ref, po_ref, c_ref, y_ref, prev_ref, k_ref, *refs):
    rows, (y_out, mo_out, mr_out, p_out) = refs[:4], refs[4:]
    y = next_inner(v_ref, part_ref, c_ref, y_ref, prev_ref, *rows[2:])
    y_out[...] = y
    inner_columns(y.astype(BF16), rows, mo_out, mr_out)
    p_out[...] = po_ref[...] + corner(rows[0], rows[1], k_ref, v_ref[...])


def side():
    return jnp.bitwise_and(lax.axis_index("band"), 1)


def last_m_kernel(v_ref, part_ref, c_ref, y_ref, prev_ref, hr_ref, lr_ref, f_out, same_out, cross_out):
    f_out[...] = next_inner(v_ref, part_ref, c_ref, y_ref, prev_ref, hr_ref, lr_ref).astype(BF16)
    half = same_out.shape[0]
    same_out[...] = f_out[at(side() * half, half), :]
    cross_out[...] = f_out[at((1 - side()) * half, half), :]


def corner_kernel(v_ref, p_ref, ho_ref, lo_ref, k_ref, p_out):
    p_out[...] = p_ref[...] + corner(ho_ref, lo_ref, k_ref, v_ref[...])


def last_kernel(re_ref, ro_ref, pe_ref, po_ref, c_ref, ye_ref, yo_ref, we_ref, wo_ref, f_ref):
    odd = is_odd()
    ext = c_ref.shape[0]
    g = re_ref.shape[0]
    base = ext - 2 * g
    here = at(jnp.where(odd, 0, g), g)
    total = po_ref[here, :] + ro_ref[...].astype(F32)
    f_ref[:g, :] = advance(c_ref[here, :] * total, yo_ref[here, :], wo_ref[here, :]).astype(BF16)
    here = at(jnp.where(odd, g, 0), g)
    total = pe_ref[here, :] + re_ref[...]
    scale = c_ref[at(base + jnp.where(odd, g, 0), g), :]
    f_ref[g:, :] = advance(scale * total, ye_ref[here, :], we_ref[here, :]).astype(BF16)


def join_kernel(fm_ref, fb_ref, out_ref):
    odd = is_odd()
    g = fb_ref.shape[0] // 2
    far = out_ref.shape[0] - g
    out_ref[g:far, :] = fm_ref[...]
    out_ref[at(jnp.where(odd, far, 0), g), :] = fb_ref[:g, :]
    out_ref[at(jnp.where(odd, 0, far), g), :] = fb_ref[g:, :]


def pack_kernel(*refs):
    out_ref = refs[-1]
    start = 0
    for ref in refs[:-1]:
        out_ref[start : start + ref.shape[0], :] = ref[...]
        start += ref.shape[0]


def gram(a, b):
    return lax.dot_general(a, b, (((0,), (0,)), ((), ())), preferred_element_type=F32)


def place(k, width):
    return at((lax.axis_index("band") ^ k) * width, width)


def margin_m_kernel(own_ref, *refs):
    out_ref = refs[-1]
    width = own_ref.shape[1]
    half = own_ref.shape[0] // 2
    own = own_ref[...]
    out_ref[:width, :] = gram(own, own)
    own = own_ref[at(side() * half, half), :]
    for i, ref in enumerate(refs[:-1]):
        out_ref[(i + 1) * width : (i + 2) * width, :] = gram(ref[...], own)


def margin_b_kernel(m_ref, b_ref, near_ref, before_ref, *refs):
    out_ref = refs[-1]
    width = m_ref.shape[1]
    inner = m_ref.shape[0]
    owned = inner + b_ref.shape[0]
    half = inner // 2
    own = b_ref[...]
    out_ref[place(0, width), :] = (before_ref[:width, :] + gram(own, own)).astype(BF16)
    block = gram(near_ref[:inner, :], m_ref[...]) + gram(near_ref[inner:owned, :], own)
    out_ref[place(1, width), :] = block.astype(BF16)
    other = m_ref[at((1 - side()) * half, half), :]
    for i, ref in enumerate(refs[:-1]):
        relayed = owned + (i ^ 1) * half
        block = before_ref[(i + 1) * width : (i + 2) * width, :] + gram(ref[...], own)
        block = block + gram(near_ref[relayed : relayed + half, :], other)
        out_ref[place(i + 2, width), :] = block.astype(BF16)


def shards(wavefunctions, cell_ham, connectivity, inv_mass, cell_count):
    owned, width = wavefunctions.shape
    cells, slots = connectivity.shape
    g = cell_ham.shape[1] // 4
    edge = 2 * g
    ext = owned + edge
    inner = ext - 2 * edge
    domains = lax.axis_size("dom")
    bands = lax.axis_size("band")
    if domains % 2 or bands & (bands - 1) or g != LANES or width != LANES or slots != 2 * edge:
        raise ValueError("unsupported sizes")
    even_pairs = [(i, i ^ 1) for i in range(domains)]
    odd_pairs = [(i, (i + 1) % domains if i % 2 else (i - 1) % domains) for i in range(domains)]

    def swap_even(x):
        return lax.ppermute(x, "dom", even_pairs)

    def swap_odd(x):
        return lax.ppermute(x, "dom", odd_pairs)

    def shift(x, k):
        return lax.ppermute(x, "band", [(i, i ^ k) for i in range(bands)])

    def flops(rows, cols):
        return 4 * rows * cols * width

    masses = inv_mass.reshape(owned // LANES, LANES)
    rim = ((g + PAD, width), BF16)
    inputs = (wavefunctions, masses, connectivity, cell_ham)
    rim_o, rim_e, wavefunctions, masses, position, cell_ham = call(
        rim_kernel,
        [rim, rim] + [(x.shape, x.dtype) for x in inputs],
        [SMEM] + [HBM] * 4,
        1 << 10,
        [pltpu.SemaphoreType.DMA((4,))],
    )(cell_count, *[pltpu.with_memory_space_constraint(x, pltpu.HBM) for x in inputs])
    halo_o = swap_odd(rim_o)
    halo_e = swap_even(rim_e)

    def block(rows, dtype=F32, cols=width):
        return ((rows, cols), dtype)

    *rows_o, pick, corner_mine = call(
        assemble_o_kernel,
        [block(edge, BF16, ext)] * 2 + [block(cells * slots, BF16, ext), block(edge, BF16, 2 * edge)],
        [VMEM] * 2,
        2 * cells * edge * slots * (slots + 2 * ext),
    )(position, cell_ham)
    corner_far = lax.ppermute(corner_mine, "dom", odd_pairs)
    rows_r = call(
        assemble_r_kernel,
        [block(ext - edge, BF16, ext)] * 2,
        [VMEM] * 3,
        2 * cells * (ext - edge) * slots * (slots + 2 * ext),
    )(position, cell_ham, pick)
    rows = (*rows_o, *rows_r)

    start, p_o, s_o = call(
        first_o_kernel,
        [block(ext, BF16), block(edge), block(edge, BF16)],
        [VMEM] * 5,
        flops(edge, ext),
    )(wavefunctions, halo_e, halo_o, *rows_o)
    r_o = swap_odd(s_o)
    (p_e,) = call(first_e_kernel, [block(edge)], [VMEM] * 3, flops(edge, ext))(start, *rows_r)
    s_e = p_e
    parts_m = [block(edge), block(ext - edge)]
    y_e = y_o = w_m = start
    w_e = w_o = v_o = y_m = part_o = part_r = None
    for step in range(1, DEGREE):
        last = step == DEGREE - 1
        first = step == 1
        r_e = swap_even(s_e)
        if first:
            scale, y_m, *middle = call(
                first_m_kernel, [block(ext), block(inner)] + parts_m, [VMEM] * 8, flops(ext, ext)
            )(start, halo_e, halo_o, masses, *rows)
        else:
            new_m, *middle, p_o = call(
                rest_m_kernel,
                [block(inner)] + parts_m + [block(edge)],
                [VMEM] * 11,
                flops(ext, ext),
            )(v_o, part_r, part_o, scale, y_m, w_m, corner_far, *rows)
            w_m, y_m = y_m, new_m
        new_e, part_o, part_r, s_o = call(
            functools.partial(even_kernel, first, last),
            [block(edge), block(edge), block(ext - edge), block(g if last else edge, BF16)],
            [VMEM] * (10 if first else 11),
            flops(ext, edge),
        )(r_e, p_e, scale, y_e, *(() if first else (w_e,)), *middle, *rows)
        r_next = swap_odd(s_o)
        new_o, v_o = call(
            functools.partial(odd_kernel, first),
            [block(edge), block(edge, BF16)],
            [VMEM] * (4 if first else 5),
            1 << 10,
        )(r_o, p_o, scale, y_o, *(() if first else (w_o,)))
        p_e, *half = call(
            rest_e_kernel, [block(edge)] + [block(g)] * last, [VMEM] * 4, flops(edge, edge)
        )(v_o, part_r, *rows_r)
        s_e = half[0] if last else p_e
        r_o = r_next
        w_e, w_o = y_e, y_o
        y_e, y_o = new_e, new_o
    r_e = swap_even(s_e)
    half = block(inner // 2, BF16)
    f_m, same, cross = call(
        last_m_kernel, [block(inner, BF16), half, half], [VMEM] * 7, flops(inner, edge)
    )(v_o, part_r, scale, y_m, w_m, *rows_r)
    far_m = [shift(cross if k % 2 else same, k) for k in range(2, bands)]
    (p_o,) = call(corner_kernel, [block(edge)], [VMEM] * 5, flops(edge, 2 * edge))(
        v_o, part_o, *rows_o, corner_far
    )
    (f_b,) = call(last_kernel, [block(edge, BF16)], [VMEM] * 9, edge * width * 8)(
        r_e, r_o, p_e, p_o, scale, y_e, y_o, w_e, w_o
    )
    far_b = [shift(f_b, k) for k in range(2, bands)]
    (packed,) = call(
        pack_kernel, [block(owned + (bands - 2) * (inner // 2), BF16)], [VMEM] * bands, 1 << 10
    )(f_m, f_b, *far_m)
    near = shift(packed, 1)
    (filtered,) = call(join_kernel, [block(owned, BF16)], [VMEM] * 2, 1 << 10)(f_m, f_b)
    total = bands * width
    (before,) = call(
        margin_m_kernel,
        [((total - width, width), F32)],
        [VMEM] * (bands - 1),
        2 * total * width * inner,
    )(f_m, *far_m)
    (sums,) = call(
        margin_b_kernel, [((total, width), BF16)], [VMEM] * (bands + 2), 2 * total * width * owned
    )(f_m, f_b, near, before, *far_b)
    parts = lax.all_to_all(sums.reshape(domains, total // domains, width), "dom", 0, 0)
    factor = 1.0 / jnp.sqrt(F32(owned * domains))
    return (filtered, (jnp.sum(parts.astype(F32), axis=0) * factor).T)


def solution(mesh):
    return jax.shard_map(
        shards,
        mesh=mesh,
        in_specs=(P("dom", "band"), P("dom", None, None), P("dom", None), P("dom"), P("dom")),
        out_specs=(P("dom", "band"), P("band", "dom")),
        check_vma=False,
    )
```

```python
import functools

import jax
import jax.numpy as jnp
from jax import lax
from jax.experimental import pallas as pl
from jax.experimental.pallas import tpu as pltpu
from jax.sharding import PartitionSpec as P


DEGREE = 4
LANES = 128
PAD = 16
VMEM_LIMIT = 16 << 20

filter_center = 0.5
filter_halfwidth = 3.0

F32 = jnp.float32
BF16 = jnp.bfloat16
VMEM = pl.BlockSpec(memory_space=pltpu.VMEM)
SMEM = pl.BlockSpec(memory_space=pltpu.SMEM)
HBM = pl.BlockSpec(memory_space=pltpu.HBM)


def call(kernel, outs, ins, flops, scratch=()):
    return pl.pallas_call(
        kernel,
        out_shape=[jax.ShapeDtypeStruct(s, d) for s, d in outs],
        in_specs=ins,
        out_specs=[VMEM] * len(outs),
        scratch_shapes=list(scratch),
        cost_estimate=pl.CostEstimate(flops=flops, bytes_accessed=1 << 20, transcendentals=0),
        compiler_params=pltpu.CompilerParams(vmem_limit_bytes=VMEM_LIMIT),
    )


def is_odd():
    return jnp.bitwise_and(lax.axis_index("dom"), 1) == 1


def at(start, size):
    return pl.ds(pl.multiple_of(start, LANES), size)


def to_columns(row):
    width = row.shape[1]
    parts = [
        jnp.broadcast_to(row[:, i : i + LANES], (LANES, LANES)).T for i in range(0, width, LANES)
    ]
    return parts[0] if len(parts) == 1 else jnp.concatenate(parts, axis=0)


def split(x):
    high = x.astype(BF16)
    return high, (x - high.astype(F32)).astype(BF16)


def dot(a, b):
    return jnp.dot(a, b, preferred_element_type=F32)


def apply(hi_ref, lo_ref, cols, values):
    return dot(hi_ref[:, cols], values) + dot(lo_ref[:, cols], values)


def advance(applied, current, previous):
    moved = (applied - filter_center * current) / filter_halfwidth
    return moved if previous is None else 2.0 * moved - previous


def rim_kernel(
    count_ref, v_hbm, d_hbm, conn_hbm, ham_hbm, ro_ref, re_ref, v_ref, d_ref, pos_ref, ham_ref, sems
):
    pairs = (
        (ham_hbm, ham_ref),
        (v_hbm, v_ref),
        (d_hbm, d_ref),
        (conn_hbm, pos_ref),
    )
    copies = [pltpu.make_async_copy(a, b, sems.at[i]) for i, (a, b) in enumerate(pairs)]
    for copy in copies[1:] + copies[:1]:
        copy.start()
    odd = is_odd()
    owned = v_ref.shape[0]
    g = ro_ref.shape[0] - PAD
    far = owned - g
    row = lax.broadcasted_iota(jnp.int32, (PAD, LANES), 0)
    for copy in copies[1:]:
        copy.wait()
    for out, edge in ((ro_ref, jnp.where(odd, far, 0)), (re_ref, jnp.where(odd, 0, far))):
        out[:g, :] = v_ref[at(edge, g), :]
        mass = d_ref[pl.ds(edge // LANES, 1), :]
        high = mass.astype(BF16).astype(F32)
        out[g:, :] = jnp.where(row == 0, high, jnp.where(row == 1, mass - high, 0.0)).astype(BF16)
    cells, slots = pos_ref.shape
    edge = slots // 2
    base = owned + 2 * g - edge
    conn = pos_ref[...]
    turned = jnp.where(conn < edge, conn + base, jnp.where(conn >= base, conn - base, conn))
    live = lax.broadcasted_iota(jnp.int32, (cells, slots), 0) < count_ref[0]
    pos_ref[...] = jnp.where(live, jnp.where(odd, turned, conn), -1)
    copies[0].wait()


def gather_rows(pos_ref, ham_ref, pick_ref, first, count):
    cells, slots = pos_ref.shape
    total = None
    for c in range(cells):
        row = pos_ref[c : c + 1, :]
        spread = lax.broadcasted_iota(jnp.int32, (count, slots), 0) + first == row
        spread = jnp.where(spread, 1.0, 0.0).astype(BF16)
        high, low = split(dot(spread, ham_ref[c]))
        pick = pick_ref[c * slots : (c + 1) * slots, :]
        part = dot(high, pick) + dot(low, pick)
        total = part if total is None else total + part
    return split(total)


def assemble_o_kernel(pos_ref, ham_ref, hi_ref, lo_ref, pick_ref, corner_ref):
    edge, ext = hi_ref.shape
    cells, slots = pos_ref.shape
    lane = lax.broadcasted_iota(jnp.int32, (slots, LANES), 1)
    for c in range(cells):
        column = to_columns(pos_ref[c : c + 1, :].astype(F32)).astype(jnp.int32)
        for i in range(0, ext, LANES):
            pick_ref[c * slots : (c + 1) * slots, i : i + LANES] = jnp.where(
                lane + i == column, 1.0, 0.0
            ).astype(BF16)
    high, low = gather_rows(pos_ref, ham_ref, pick_ref, 0, edge)
    hi_ref[...] = high
    lo_ref[...] = low
    corner_ref[:, :edge] = high[:, :edge]
    corner_ref[:, edge:] = low[:, :edge]


def assemble_r_kernel(pos_ref, ham_ref, pick_ref, hi_ref, lo_ref):
    rest, ext = hi_ref.shape
    hi_ref[...], lo_ref[...] = gather_rows(pos_ref, ham_ref, pick_ref, ext - rest, rest)


def first_o_kernel(v_ref, he_ref, ho_ref, hi_ref, lo_ref, vx_ref, p_ref, s_ref):
    odd = is_odd()
    owned = v_ref.shape[0]
    ext = hi_ref.shape[1]
    g = (ext - owned) // 2
    base = ext - 2 * g
    far = owned - g
    vx_ref[at(jnp.where(odd, g, 0), g), :] = ho_ref[:g, :]
    vx_ref[at(jnp.where(odd, 0, g), g), :] = v_ref[at(jnp.where(odd, far, 0), g), :]
    vx_ref[2 * g : base, :] = v_ref[g:far, :]
    vx_ref[at(base + jnp.where(odd, 0, g), g), :] = he_ref[:g, :]
    vx_ref[at(base + jnp.where(odd, g, 0), g), :] = v_ref[at(jnp.where(odd, 0, far), g), :]
    product = apply(hi_ref, lo_ref, slice(None), vx_ref[...])
    p_ref[...] = product
    s_ref[...] = product.astype(BF16)


def first_e_kernel(vx_ref, hi_ref, lo_ref, p_ref):
    edge = p_ref.shape[0]
    rest = hi_ref.shape[0]
    values = vx_ref[...]
    p_ref[...] = dot(hi_ref[rest - edge :, :], values) + dot(lo_ref[rest - edge :, :], values)


def inner_columns(v, rows, mo_out, mr_out):
    ho_ref, lo_ref, hr_ref, lr_ref = rows
    edge = ho_ref.shape[0]
    inner = slice(edge, edge + v.shape[0])
    mo_out[...] = apply(ho_ref, lo_ref, inner, v)
    mr_out[...] = apply(hr_ref, lr_ref, inner, v)


def first_m_kernel(vx_ref, he_ref, ho_ref, d_ref, *refs):
    rows, (c_ref, y_out, mo_out, mr_out) = refs[:4], refs[4:]
    hr_ref, lr_ref = rows[2:]
    odd = is_odd()
    ext = hr_ref.shape[1]
    g = he_ref.shape[0] - PAD
    owned = ext - 2 * g
    base = ext - 2 * g
    far = owned - g

    def mass(ref):
        return to_columns(jnp.sum(ref[g:, :].astype(F32), axis=0, keepdims=True))

    def own(block):
        return to_columns(d_ref[pl.ds(block, 1), :])

    c_ref[at(jnp.where(odd, g, 0), g), :] = mass(ho_ref)
    c_ref[at(jnp.where(odd, 0, g), g), :] = own(jnp.where(odd, far // LANES, 0))
    for i in range(1, far // LANES):
        c_ref[g + i * LANES : g + (i + 1) * LANES, :] = own(i)
    c_ref[at(base + jnp.where(odd, 0, g), g), :] = mass(he_ref)
    c_ref[at(base + jnp.where(odd, g, 0), g), :] = own(jnp.where(odd, 0, far // LANES))
    middle = slice(2 * g, base)
    inner = base - 2 * g
    values = vx_ref[...]
    product = dot(hr_ref[:inner, :], values) + dot(lr_ref[:inner, :], values)
    y = advance(c_ref[middle, :] * product, vx_ref[middle, :].astype(F32), None)
    y_out[...] = y
    inner_columns(y.astype(BF16), rows, mo_out, mr_out)


def even_kernel(
    first, last, r_ref, p_ref, c_ref, y_ref, *rest
):
    rest = list(rest)
    prev_ref = None if first else rest.pop(0)
    mo_ref, mr_ref, ho_ref, lo_ref, hr_ref, lr_ref, y_out, po_out, pr_out, s_out = rest
    ext = ho_ref.shape[1]
    edge = r_ref.shape[0]
    block = slice(ext - edge, ext)
    current = y_ref[block, :].astype(F32) if first else y_ref[...]
    previous = None if first else tail(prev_ref, edge)
    y = advance(c_ref[block, :] * (p_ref[...] + r_ref[...]), current, previous)
    y_out[...] = y
    values = y.astype(BF16)
    part = mo_ref[...] + apply(ho_ref, lo_ref, block, values)
    po_out[...] = part
    if last:
        g = s_out.shape[0]
        s_out[...] = po_out[at(jnp.where(is_odd(), g, 0), g), :].astype(BF16)
    else:
        s_out[...] = part.astype(BF16)
    pr_out[...] = mr_ref[...] + apply(hr_ref, lr_ref, block, values)


def tail(ref, size):
    return ref[ref.shape[0] - size :, :].astype(F32)


def head(ref, size):
    return ref[:size, :].astype(F32)


def corner(ho_ref, lo_ref, k_ref, values):
    edge = values.shape[0]
    return (
        apply(ho_ref, lo_ref, slice(0, edge), values)
        + dot(k_ref[:, :edge], values)
        + dot(k_ref[:, edge:], values)
    )


def odd_kernel(first, r_ref, p_ref, c_ref, y_ref, *rest):
    y_out, v_out = rest[-2:]
    edge = r_ref.shape[0]
    total = p_ref[...] + r_ref[...].astype(F32)
    previous = None if first else head(rest[0], edge)
    y = advance(c_ref[:edge, :] * total, head(y_ref, edge), previous)
    y_out[...] = y
    v_out[...] = y.astype(BF16)


def rest_e_kernel(v_ref, part_ref, hr_ref, lr_ref, p_out, *s_out):
    edge = v_ref.shape[0]
    rows = slice(hr_ref.shape[0] - edge, hr_ref.shape[0])
    values = v_ref[...]
    p_out[...] = (
        part_ref[rows, :]
        + dot(hr_ref[rows, :edge], values)
        + dot(lr_ref[rows, :edge], values)
    )
    if s_out:
        g = s_out[0].shape[0]
        s_out[0][...] = p_out[at(jnp.where(is_odd(), 0, g), g), :]


def next_inner(v_ref, part_ref, c_ref, y_ref, prev_ref, hr_ref, lr_ref):
    ext = hr_ref.shape[1]
    edge = v_ref.shape[0]
    inner = y_ref.shape[0]
    values = v_ref[...]
    product = (
        part_ref[:inner, :] + dot(hr_ref[:inner, :edge], values) + dot(lr_ref[:inner, :edge], values)
    )
    middle = slice(edge, edge + inner)
    previous = prev_ref[middle, :].astype(F32) if prev_ref.shape[0] == ext else prev_ref[...]
    return advance(c_ref[middle, :] * product, y_ref[...], previous)


def rest_m_kernel(v_ref, part_ref, po_ref, c_ref, y_ref, prev_ref, k_ref, *refs):
    rows, (y_out, mo_out, mr_out, p_out) = refs[:4], refs[4:]
    y = next_inner(v_ref, part_ref, c_ref, y_ref, prev_ref, *rows[2:])
    y_out[...] = y
    inner_columns(y.astype(BF16), rows, mo_out, mr_out)
    p_out[...] = po_ref[...] + corner(rows[0], rows[1], k_ref, v_ref[...])


def side():
    return jnp.bitwise_and(lax.axis_index("band"), 1)


def last_m_kernel(v_ref, part_ref, c_ref, y_ref, prev_ref, hr_ref, lr_ref, f_out, same_out, cross_out):
    f_out[...] = next_inner(v_ref, part_ref, c_ref, y_ref, prev_ref, hr_ref, lr_ref).astype(BF16)
    half = same_out.shape[0]
    same_out[...] = f_out[at(side() * half, half), :]
    cross_out[...] = f_out[at((1 - side()) * half, half), :]


def corner_kernel(v_ref, p_ref, ho_ref, lo_ref, k_ref, p_out):
    p_out[...] = p_ref[...] + corner(ho_ref, lo_ref, k_ref, v_ref[...])


def last_kernel(re_ref, ro_ref, pe_ref, po_ref, c_ref, ye_ref, yo_ref, we_ref, wo_ref, fm_ref, f_ref, all_ref):
    odd = is_odd()
    ext = c_ref.shape[0]
    g = re_ref.shape[0]
    base = ext - 2 * g
    here = at(jnp.where(odd, 0, g), g)
    total = po_ref[here, :] + ro_ref[...].astype(F32)
    f_ref[:g, :] = advance(c_ref[here, :] * total, yo_ref[here, :], wo_ref[here, :]).astype(BF16)
    here = at(jnp.where(odd, g, 0), g)
    total = pe_ref[here, :] + re_ref[...]
    scale = c_ref[at(base + jnp.where(odd, g, 0), g), :]
    f_ref[g:, :] = advance(scale * total, ye_ref[here, :], we_ref[here, :]).astype(BF16)
    inner = fm_ref.shape[0]
    all_ref[:inner, :] = fm_ref[...]
    all_ref[inner:, :] = f_ref[...]


def join_kernel(fm_ref, fb_ref, out_ref):
    odd = is_odd()
    g = fb_ref.shape[0] // 2
    far = out_ref.shape[0] - g
    out_ref[g:far, :] = fm_ref[...]
    out_ref[at(jnp.where(odd, far, 0), g), :] = fb_ref[:g, :]
    out_ref[at(jnp.where(odd, 0, far), g), :] = fb_ref[g:, :]


def pack_kernel(*refs):
    out_ref = refs[-1]
    start = 0
    for ref in refs[:-1]:
        out_ref[start : start + ref.shape[0], :] = ref[...]
        start += ref.shape[0]


def gram(a, b):
    return lax.dot_general(a, b, (((0,), (0,)), ((), ())), preferred_element_type=F32)


def place(k, width):
    return at((lax.axis_index("band") ^ k) * width, width)


def margin_m_kernel(own_ref, *refs):
    out_ref = refs[-1]
    width = own_ref.shape[1]
    half = own_ref.shape[0] // 2
    own = own_ref[...]
    out_ref[:width, :] = gram(own, own)
    own = own_ref[at(side() * half, half), :]
    for i, ref in enumerate(refs[:-1]):
        out_ref[(i + 1) * width : (i + 2) * width, :] = gram(ref[...], own)


def margin_b_kernel(m_ref, b_ref, near_ref, relay_ref, before_ref, *refs):
    out_ref = refs[-1]
    width = m_ref.shape[1]
    inner = m_ref.shape[0]
    owned = inner + b_ref.shape[0]
    half = inner // 2
    own = b_ref[...]
    out_ref[place(0, width), :] = (before_ref[:width, :] + gram(own, own)).astype(BF16)
    block = gram(near_ref[:inner, :], m_ref[...]) + gram(near_ref[inner:owned, :], own)
    out_ref[place(1, width), :] = block.astype(BF16)
    other = m_ref[at((1 - side()) * half, half), :]
    for i, ref in enumerate(refs[:-1]):
        relayed = (i ^ 1) * half
        block = before_ref[(i + 1) * width : (i + 2) * width, :] + gram(ref[...], own)
        block = block + gram(relay_ref[relayed : relayed + half, :], other)
        out_ref[place(i + 2, width), :] = block.astype(BF16)


def shards(wavefunctions, cell_ham, connectivity, inv_mass, cell_count):
    owned, width = wavefunctions.shape
    cells, slots = connectivity.shape
    g = cell_ham.shape[1] // 4
    edge = 2 * g
    ext = owned + edge
    inner = ext - 2 * edge
    domains = lax.axis_size("dom")
    bands = lax.axis_size("band")
    if domains % 2 or bands & (bands - 1) or g != LANES or width != LANES or slots != 2 * edge:
        raise ValueError("unsupported sizes")
    even_pairs = [(i, i ^ 1) for i in range(domains)]
    odd_pairs = [(i, (i + 1) % domains if i % 2 else (i - 1) % domains) for i in range(domains)]

    def swap_even(x):
        return lax.ppermute(x, "dom", even_pairs)

    def swap_odd(x):
        return lax.ppermute(x, "dom", odd_pairs)

    def shift(x, k):
        return lax.ppermute(x, "band", [(i, i ^ k) for i in range(bands)])

    def flops(rows, cols):
        return 4 * rows * cols * width

    masses = inv_mass.reshape(owned // LANES, LANES)
    rim = ((g + PAD, width), BF16)
    inputs = (wavefunctions, masses, connectivity, cell_ham)
    rim_o, rim_e, wavefunctions, masses, position, cell_ham = call(
        rim_kernel,
        [rim, rim] + [(x.shape, x.dtype) for x in inputs],
        [SMEM] + [HBM] * 4,
        1 << 10,
        [pltpu.SemaphoreType.DMA((4,))],
    )(cell_count, *[pltpu.with_memory_space_constraint(x, pltpu.HBM) for x in inputs])
    halo_o = swap_odd(rim_o)
    halo_e = swap_even(rim_e)

    def block(rows, dtype=F32, cols=width):
        return ((rows, cols), dtype)

    *rows_o, pick, corner_mine = call(
        assemble_o_kernel,
        [block(edge, BF16, ext)] * 2 + [block(cells * slots, BF16, ext), block(edge, BF16, 2 * edge)],
        [VMEM] * 2,
        2 * cells * edge * slots * (slots + 2 * ext),
    )(position, cell_ham)
    corner_far = lax.ppermute(corner_mine, "dom", odd_pairs)
    rows_r = call(
        assemble_r_kernel,
        [block(ext - edge, BF16, ext)] * 2,
        [VMEM] * 3,
        2 * cells * (ext - edge) * slots * (slots + 2 * ext),
    )(position, cell_ham, pick)
    rows = (*rows_o, *rows_r)

    start, p_o, s_o = call(
        first_o_kernel,
        [block(ext, BF16), block(edge), block(edge, BF16)],
        [VMEM] * 5,
        flops(edge, ext),
    )(wavefunctions, halo_e, halo_o, *rows_o)
    r_o = swap_odd(s_o)
    (p_e,) = call(first_e_kernel, [block(edge)], [VMEM] * 3, flops(edge, ext))(start, *rows_r)
    s_e = p_e
    parts_m = [block(edge), block(ext - edge)]
    y_e = y_o = w_m = start
    w_e = w_o = v_o = y_m = part_o = part_r = None
    for step in range(1, DEGREE):
        last = step == DEGREE - 1
        first = step == 1
        r_e = swap_even(s_e)
        if first:
            scale, y_m, *middle = call(
                first_m_kernel, [block(ext), block(inner)] + parts_m, [VMEM] * 8, flops(ext, ext)
            )(start, halo_e, halo_o, masses, *rows)
        else:
            new_m, *middle, p_o = call(
                rest_m_kernel,
                [block(inner)] + parts_m + [block(edge)],
                [VMEM] * 11,
                flops(ext, ext),
            )(v_o, part_r, part_o, scale, y_m, w_m, corner_far, *rows)
            w_m, y_m = y_m, new_m
        new_e, part_o, part_r, s_o = call(
            functools.partial(even_kernel, first, last),
            [block(edge), block(edge), block(ext - edge), block(g if last else edge, BF16)],
            [VMEM] * (10 if first else 11),
            flops(ext, edge),
        )(r_e, p_e, scale, y_e, *(() if first else (w_e,)), *middle, *rows)
        r_next = swap_odd(s_o)
        new_o, v_o = call(
            functools.partial(odd_kernel, first),
            [block(edge), block(edge, BF16)],
            [VMEM] * (4 if first else 5),
            1 << 10,
        )(r_o, p_o, scale, y_o, *(() if first else (w_o,)))
        p_e, *half = call(
            rest_e_kernel, [block(edge)] + [block(g)] * last, [VMEM] * 4, flops(edge, edge)
        )(v_o, part_r, *rows_r)
        s_e = half[0] if last else p_e
        r_o = r_next
        w_e, w_o = y_e, y_o
        y_e, y_o = new_e, new_o
    r_e = swap_even(s_e)
    half = block(inner // 2, BF16)
    f_m, same, cross = call(
        last_m_kernel, [block(inner, BF16), half, half], [VMEM] * 7, flops(inner, edge)
    )(v_o, part_r, scale, y_m, w_m, *rows_r)
    far_m = [shift(cross if k % 2 else same, k) for k in range(2, bands)]
    (p_o,) = call(corner_kernel, [block(edge)], [VMEM] * 5, flops(edge, 2 * edge))(
        v_o, part_o, *rows_o, corner_far
    )
    f_b, f_all = call(
        last_kernel, [block(edge, BF16), block(owned, BF16)], [VMEM] * 10, edge * width * 8
    )(
        r_e, r_o, p_e, p_o, scale, y_e, y_o, w_e, w_o, f_m
    )
    far_b = [shift(f_b, k) for k in range(2, bands)]
    (packed,) = call(
        pack_kernel, [block((bands - 2) * (inner // 2), BF16)], [VMEM] * (bands - 2), 1 << 10
    )(*far_m)
    near = shift(f_all, 1)
    relayed = shift(packed, 1)
    (filtered,) = call(join_kernel, [block(owned, BF16)], [VMEM] * 2, 1 << 10)(f_m, f_b)
    total = bands * width
    (before,) = call(
        margin_m_kernel,
        [((total - width, width), F32)],
        [VMEM] * (bands - 1),
        2 * total * width * inner,
    )(f_m, *far_m)
    (sums,) = call(
        margin_b_kernel, [((total, width), BF16)], [VMEM] * (bands + 3), 2 * total * width * owned
    )(f_m, f_b, near, relayed, before, *far_b)
    parts = lax.all_to_all(sums.reshape(domains, total // domains, width), "dom", 0, 0)
    factor = 1.0 / jnp.sqrt(F32(owned * domains))
    return (filtered, (jnp.sum(parts.astype(F32), axis=0) * factor).T)


def solution(mesh):
    return jax.shard_map(
        shards,
        mesh=mesh,
        in_specs=(P("dom", "band"), P("dom", None, None), P("dom", None), P("dom"), P("dom")),
        out_specs=(P("dom", "band"), P("band", "dom")),
        check_vma=False,
    )
```

```python
import functools

import jax
import jax.numpy as jnp
from jax import lax
from jax.experimental import pallas as pl
from jax.experimental.pallas import tpu as pltpu
from jax.sharding import PartitionSpec as P


DEGREE = 4
LANES = 128
PAD = 16
VMEM_LIMIT = 16 << 20

filter_center = 0.5
filter_halfwidth = 3.0

F32 = jnp.float32
BF16 = jnp.bfloat16
VMEM = pl.BlockSpec(memory_space=pltpu.VMEM)
SMEM = pl.BlockSpec(memory_space=pltpu.SMEM)
HBM = pl.BlockSpec(memory_space=pltpu.HBM)


def call(kernel, outs, ins, flops, scratch=()):
    return pl.pallas_call(
        kernel,
        out_shape=[jax.ShapeDtypeStruct(s, d) for s, d in outs],
        in_specs=ins,
        out_specs=[VMEM] * len(outs),
        scratch_shapes=list(scratch),
        cost_estimate=pl.CostEstimate(flops=flops, bytes_accessed=1 << 20, transcendentals=0),
        compiler_params=pltpu.CompilerParams(vmem_limit_bytes=VMEM_LIMIT),
    )


def is_odd():
    return jnp.bitwise_and(lax.axis_index("dom"), 1) == 1


def at(start, size):
    return pl.ds(pl.multiple_of(start, LANES), size)


def to_columns(row):
    width = row.shape[1]
    parts = [
        jnp.broadcast_to(row[:, i : i + LANES], (LANES, LANES)).T for i in range(0, width, LANES)
    ]
    return parts[0] if len(parts) == 1 else jnp.concatenate(parts, axis=0)


def split(x):
    high = x.astype(BF16)
    return high, (x - high.astype(F32)).astype(BF16)


def dot(a, b):
    return jnp.dot(a, b, preferred_element_type=F32)


def apply(hi_ref, lo_ref, cols, values):
    return dot(hi_ref[:, cols], values) + dot(lo_ref[:, cols], values)


def advance(applied, current, previous):
    moved = (applied - filter_center * current) / filter_halfwidth
    return moved if previous is None else 2.0 * moved - previous


def rim_kernel(
    count_ref, v_hbm, d_hbm, conn_hbm, ham_hbm, ro_ref, re_ref, v_ref, d_ref, pos_ref, ham_ref, sems
):
    pairs = (
        (ham_hbm, ham_ref),
        (v_hbm, v_ref),
        (d_hbm, d_ref),
        (conn_hbm, pos_ref),
    )
    copies = [pltpu.make_async_copy(a, b, sems.at[i]) for i, (a, b) in enumerate(pairs)]
    for copy in copies[1:] + copies[:1]:
        copy.start()
    odd = is_odd()
    owned = v_ref.shape[0]
    g = ro_ref.shape[0] - PAD
    far = owned - g
    row = lax.broadcasted_iota(jnp.int32, (PAD, LANES), 0)
    for copy in copies[1:]:
        copy.wait()
    for out, edge in ((ro_ref, jnp.where(odd, far, 0)), (re_ref, jnp.where(odd, 0, far))):
        out[:g, :] = v_ref[at(edge, g), :]
        mass = d_ref[pl.ds(edge // LANES, 1), :]
        high = mass.astype(BF16).astype(F32)
        out[g:, :] = jnp.where(row == 0, high, jnp.where(row == 1, mass - high, 0.0)).astype(BF16)
    cells, slots = pos_ref.shape
    edge = slots // 2
    base = owned + 2 * g - edge
    conn = pos_ref[...]
    turned = jnp.where(conn < edge, conn + base, jnp.where(conn >= base, conn - base, conn))
    live = lax.broadcasted_iota(jnp.int32, (cells, slots), 0) < count_ref[0]
    pos_ref[...] = jnp.where(live, jnp.where(odd, turned, conn), -1)
    copies[0].wait()


def gather_rows(pos_ref, ham_ref, pick_ref, first, count):
    cells, slots = pos_ref.shape
    total = None
    for c in range(cells):
        row = pos_ref[c : c + 1, :]
        spread = lax.broadcasted_iota(jnp.int32, (count, slots), 0) + first == row
        spread = jnp.where(spread, 1.0, 0.0).astype(BF16)
        high, low = split(dot(spread, ham_ref[c]))
        pick = pick_ref[c * slots : (c + 1) * slots, :]
        part = dot(high, pick) + dot(low, pick)
        total = part if total is None else total + part
    return split(total)


def assemble_om_kernel(pos_ref, ham_ref, ho_ref, lo_ref, hm_ref, lm_ref, pick_ref, corner_ref):
    edge, ext = ho_ref.shape
    inner = hm_ref.shape[0]
    cells, slots = pos_ref.shape
    lane = lax.broadcasted_iota(jnp.int32, (slots, LANES), 1)
    for c in range(cells):
        column = to_columns(pos_ref[c : c + 1, :].astype(F32)).astype(jnp.int32)
        for i in range(0, ext, LANES):
            pick_ref[c * slots : (c + 1) * slots, i : i + LANES] = jnp.where(
                lane + i == column, 1.0, 0.0
            ).astype(BF16)
    high, low = gather_rows(pos_ref, ham_ref, pick_ref, 0, edge + inner)
    ho_ref[...] = high[:edge]
    lo_ref[...] = low[:edge]
    hm_ref[...] = high[edge:]
    lm_ref[...] = low[edge:]
    corner_ref[...] = high[:edge, :edge]


def assemble_e_kernel(pos_ref, ham_ref, pick_ref, he_ref, le_ref):
    edge, ext = he_ref.shape
    he_ref[...], le_ref[...] = gather_rows(pos_ref, ham_ref, pick_ref, ext - edge, edge)


def first_o_kernel(v_ref, he_ref, ho_ref, hi_ref, lo_ref, vx_ref, p_ref, s_ref):
    odd = is_odd()
    owned = v_ref.shape[0]
    ext = hi_ref.shape[1]
    g = (ext - owned) // 2
    base = ext - 2 * g
    far = owned - g
    vx_ref[at(jnp.where(odd, g, 0), g), :] = ho_ref[:g, :]
    vx_ref[at(jnp.where(odd, 0, g), g), :] = v_ref[at(jnp.where(odd, far, 0), g), :]
    vx_ref[2 * g : base, :] = v_ref[g:far, :]
    vx_ref[at(base + jnp.where(odd, 0, g), g), :] = he_ref[:g, :]
    vx_ref[at(base + jnp.where(odd, g, 0), g), :] = v_ref[at(jnp.where(odd, 0, far), g), :]
    product = apply(hi_ref, lo_ref, slice(None), vx_ref[...])
    p_ref[...] = product
    s_ref[...] = product.astype(BF16)


def first_e_kernel(vx_ref, hi_ref, lo_ref, p_ref):
    p_ref[...] = apply(hi_ref, lo_ref, slice(None), vx_ref[...])


def columns(cols, v, rows, outs, before=(None, None, None)):
    for i, (out, part) in enumerate(zip(outs, before)):
        product = apply(rows[2 * i], rows[2 * i + 1], cols, v)
        out[...] = product if part is None else part[...] + product


def inner_columns(v, rows, outs):
    edge = rows[0].shape[0]
    columns(slice(edge, edge + v.shape[0]), v, rows, outs)


def first_m_kernel(vx_ref, he_ref, ho_ref, d_ref, *refs):
    rows, (c_ref, y_out), outs = refs[:6], refs[6:8], refs[8:]
    hm_ref, lm_ref = rows[2:4]
    odd = is_odd()
    ext = hm_ref.shape[1]
    g = he_ref.shape[0] - PAD
    owned = ext - 2 * g
    base = ext - 2 * g
    far = owned - g

    def mass(ref):
        return to_columns(jnp.sum(ref[g:, :].astype(F32), axis=0, keepdims=True))

    def own(block):
        return to_columns(d_ref[pl.ds(block, 1), :])

    c_ref[at(jnp.where(odd, g, 0), g), :] = mass(ho_ref)
    c_ref[at(jnp.where(odd, 0, g), g), :] = own(jnp.where(odd, far // LANES, 0))
    for i in range(1, far // LANES):
        c_ref[g + i * LANES : g + (i + 1) * LANES, :] = own(i)
    c_ref[at(base + jnp.where(odd, 0, g), g), :] = mass(he_ref)
    c_ref[at(base + jnp.where(odd, g, 0), g), :] = own(jnp.where(odd, 0, far // LANES))
    middle = slice(2 * g, base)
    product = apply(hm_ref, lm_ref, slice(None), vx_ref[...])
    y = advance(c_ref[middle, :] * product, vx_ref[middle, :].astype(F32), None)
    y_out[...] = y
    inner_columns(y.astype(BF16), rows, outs)


def even_kernel(first, last, r_ref, p_ref, c_ref, y_ref, *rest):
    rest = list(rest)
    prev_ref = None if first else rest.pop(0)
    before, rows, y_out, outs, s_out = rest[:3], rest[3:9], rest[9], rest[10:13], rest[13]
    ext = rows[0].shape[1]
    edge = r_ref.shape[0]
    block = slice(ext - edge, ext)
    current = y_ref[block, :].astype(F32) if first else y_ref[...]
    previous = None if first else tail(prev_ref, edge)
    y = advance(c_ref[block, :] * (p_ref[...] + r_ref[...]), current, previous)
    y_out[...] = y
    columns(block, y.astype(BF16), rows, outs, before)
    if last:
        g = s_out.shape[0]
        s_out[...] = outs[0][at(jnp.where(is_odd(), g, 0), g), :].astype(BF16)
    else:
        s_out[...] = outs[0][...].astype(BF16)


def tail(ref, size):
    return ref[ref.shape[0] - size :, :].astype(F32)


def head(ref, size):
    return ref[:size, :].astype(F32)


def corner(ho_ref, lo_ref, k_ref, values):
    return apply(ho_ref, lo_ref, slice(0, values.shape[0]), values) + dot(k_ref[...], values)


def odd_kernel(first, r_ref, p_ref, c_ref, y_ref, *rest):
    y_out, v_out = rest[-2:]
    edge = r_ref.shape[0]
    total = p_ref[...] + r_ref[...].astype(F32)
    previous = None if first else head(rest[0], edge)
    y = advance(c_ref[:edge, :] * total, head(y_ref, edge), previous)
    y_out[...] = y
    v_out[...] = y.astype(BF16)


def rest_e_kernel(v_ref, part_ref, he_ref, le_ref, p_out, *s_out):
    edge = v_ref.shape[0]
    p_out[...] = part_ref[...] + apply(he_ref, le_ref, slice(0, edge), v_ref[...])
    if s_out:
        g = s_out[0].shape[0]
        s_out[0][...] = p_out[at(jnp.where(is_odd(), 0, g), g), :]


def next_inner(v_ref, part_ref, c_ref, y_ref, prev_ref, hm_ref, lm_ref):
    ext = hm_ref.shape[1]
    edge = v_ref.shape[0]
    product = part_ref[...] + apply(hm_ref, lm_ref, slice(0, edge), v_ref[...])
    middle = slice(edge, edge + y_ref.shape[0])
    previous = prev_ref[middle, :].astype(F32) if prev_ref.shape[0] == ext else prev_ref[...]
    return advance(c_ref[middle, :] * product, y_ref[...], previous)


def rest_m_kernel(v_ref, part_ref, po_ref, c_ref, y_ref, prev_ref, k_ref, *refs):
    rows, y_out, outs, p_out = refs[:6], refs[6], refs[7:10], refs[10]
    y = next_inner(v_ref, part_ref, c_ref, y_ref, prev_ref, *rows[2:4])
    y_out[...] = y
    inner_columns(y.astype(BF16), rows, outs)
    p_out[...] = po_ref[...] + corner(rows[0], rows[1], k_ref, v_ref[...])


def last_m_kernel(v_ref, part_ref, c_ref, y_ref, prev_ref, hm_ref, lm_ref, f_out):
    f_out[...] = next_inner(v_ref, part_ref, c_ref, y_ref, prev_ref, hm_ref, lm_ref).astype(BF16)


def corner_kernel(v_ref, p_ref, ho_ref, lo_ref, k_ref, p_out):
    p_out[...] = p_ref[...] + corner(ho_ref, lo_ref, k_ref, v_ref[...])


def last_kernel(re_ref, ro_ref, pe_ref, po_ref, c_ref, ye_ref, yo_ref, we_ref, wo_ref, fm_ref, f_ref, all_ref):
    odd = is_odd()
    ext = c_ref.shape[0]
    g = re_ref.shape[0]
    base = ext - 2 * g
    here = at(jnp.where(odd, 0, g), g)
    total = po_ref[here, :] + ro_ref[...].astype(F32)
    f_ref[:g, :] = advance(c_ref[here, :] * total, yo_ref[here, :], wo_ref[here, :]).astype(BF16)
    here = at(jnp.where(odd, g, 0), g)
    total = pe_ref[here, :] + re_ref[...]
    scale = c_ref[at(base + jnp.where(odd, g, 0), g), :]
    f_ref[g:, :] = advance(scale * total, ye_ref[here, :], we_ref[here, :]).astype(BF16)
    inner = fm_ref.shape[0]
    all_ref[:inner, :] = fm_ref[...]
    all_ref[inner:, :] = f_ref[...]


def join_kernel(all_ref, out_ref):
    odd = is_odd()
    g = LANES
    far = out_ref.shape[0] - g
    inner = far - g
    out_ref[g:far, :] = all_ref[:inner, :]
    out_ref[at(jnp.where(odd, far, 0), g), :] = all_ref[inner : inner + g, :]
    out_ref[at(jnp.where(odd, 0, far), g), :] = all_ref[inner + g :, :]


def gram(a, b):
    return lax.dot_general(a, b, (((0,), (0,)), ((), ())), preferred_element_type=F32)


def place(k, width):
    return at((lax.axis_index("band") ^ k) * width, width)


def margin_m_kernel(own_ref, *refs):
    out_ref = refs[-1]
    width = own_ref.shape[1]
    for i, ref in enumerate(refs[:-1]):
        out_ref[i * width : (i + 1) * width, :] = gram(ref[...], own_ref[...])


def margin_b_kernel(all_ref, near_ref, before_ref, own_ref, *refs):
    out_ref = refs[-1]
    width = own_ref.shape[1]
    out_ref[place(0, width), :] = gram(all_ref[...], all_ref[...]).astype(BF16)
    out_ref[place(1, width), :] = gram(near_ref[...], all_ref[...]).astype(BF16)
    for i, ref in enumerate(refs[:-1]):
        block = before_ref[i * width : (i + 1) * width, :] + gram(ref[...], own_ref[...])
        out_ref[place(i + 2, width), :] = block.astype(BF16)


def shards(wavefunctions, cell_ham, connectivity, inv_mass, cell_count):
    owned, width = wavefunctions.shape
    cells, slots = connectivity.shape
    g = cell_ham.shape[1] // 4
    edge = 2 * g
    ext = owned + edge
    inner = ext - 2 * edge
    domains = lax.axis_size("dom")
    bands = lax.axis_size("band")
    if domains % 2 or bands & (bands - 1) or g != LANES or width != LANES or slots != 2 * edge:
        raise ValueError("unsupported sizes")
    even_pairs = [(i, i ^ 1) for i in range(domains)]
    odd_pairs = [(i, (i + 1) % domains if i % 2 else (i - 1) % domains) for i in range(domains)]

    def swap_even(x):
        return lax.ppermute(x, "dom", even_pairs)

    def swap_odd(x):
        return lax.ppermute(x, "dom", odd_pairs)

    def shift(x, k):
        return lax.ppermute(x, "band", [(i, i ^ k) for i in range(bands)])

    def flops(rows, cols):
        return 4 * rows * cols * width

    masses = inv_mass.reshape(owned // LANES, LANES)
    rim = ((g + PAD, width), BF16)
    inputs = (wavefunctions, masses, connectivity, cell_ham)
    rim_o, rim_e, wavefunctions, masses, position, cell_ham = call(
        rim_kernel,
        [rim, rim] + [(x.shape, x.dtype) for x in inputs],
        [SMEM] + [HBM] * 4,
        1 << 10,
        [pltpu.SemaphoreType.DMA((4,))],
    )(cell_count, *[pltpu.with_memory_space_constraint(x, pltpu.HBM) for x in inputs])
    halo_o = swap_odd(rim_o)
    halo_e = swap_even(rim_e)

    def block(rows, dtype=F32, cols=width):
        return ((rows, cols), dtype)

    *rows_om, pick, corner_mine = call(
        assemble_om_kernel,
        [block(edge, BF16, ext)] * 2
        + [block(inner, BF16, ext)] * 2
        + [block(cells * slots, BF16, ext), block(edge, BF16, edge)],
        [VMEM] * 2,
        2 * cells * (edge + inner) * slots * (slots + 2 * ext),
    )(position, cell_ham)
    rows_o, rows_m = rows_om[:2], rows_om[2:]
    start, p_o, s_o = call(
        first_o_kernel,
        [block(ext, BF16), block(edge), block(edge, BF16)],
        [VMEM] * 5,
        flops(edge, ext),
    )(wavefunctions, halo_e, halo_o, *rows_o)
    r_o = swap_odd(s_o)
    corner_far = lax.ppermute(corner_mine, "dom", odd_pairs)
    rows_e = call(
        assemble_e_kernel,
        [block(edge, BF16, ext)] * 2,
        [VMEM] * 3,
        2 * cells * edge * slots * (slots + 2 * ext),
    )(position, cell_ham, pick)
    rows = (*rows_o, *rows_m, *rows_e)

    (p_e,) = call(first_e_kernel, [block(edge)], [VMEM] * 3, flops(edge, ext))(start, *rows_e)
    s_e = p_e
    thirds = [block(edge), block(inner), block(edge)]
    y_e = y_o = w_m = start
    w_e = w_o = v_o = y_m = part_o = part_m = part_e = None
    for step in range(1, DEGREE):
        last = step == DEGREE - 1
        first = step == 1
        r_e = swap_even(s_e)
        if first:
            scale, y_m, *middle = call(
                first_m_kernel, [block(ext), block(inner)] + thirds, [VMEM] * 10, flops(ext, ext)
            )(start, halo_e, halo_o, masses, *rows)
        else:
            new_m, *middle, p_o = call(
                rest_m_kernel, [block(inner)] + thirds + [block(edge)], [VMEM] * 13, flops(ext, ext)
            )(v_o, part_m, part_o, scale, y_m, w_m, corner_far, *rows)
            w_m, y_m = y_m, new_m
        new_e, part_o, part_m, part_e, s_o = call(
            functools.partial(even_kernel, first, last),
            [block(edge)] + thirds + [block(g if last else edge, BF16)],
            [VMEM] * (13 if first else 14),
            flops(ext, edge),
        )(r_e, p_e, scale, y_e, *(() if first else (w_e,)), *middle, *rows)
        r_next = swap_odd(s_o)
        new_o, v_o = call(
            functools.partial(odd_kernel, first),
            [block(edge), block(edge, BF16)],
            [VMEM] * (4 if first else 5),
            1 << 10,
        )(r_o, p_o, scale, y_o, *(() if first else (w_o,)))
        p_e, *half = call(
            rest_e_kernel, [block(edge)] + [block(g)] * last, [VMEM] * 4, flops(edge, edge)
        )(v_o, part_e, *rows_e)
        s_e = half[0] if last else p_e
        r_o = r_next
        w_e, w_o = y_e, y_o
        y_e, y_o = new_e, new_o
    r_e = swap_even(s_e)
    (f_m,) = call(last_m_kernel, [block(inner, BF16)], [VMEM] * 7, flops(inner, edge))(
        v_o, part_m, scale, y_m, w_m, *rows_m
    )
    far_m = [shift(f_m, k) for k in range(2, bands)]
    (p_o,) = call(corner_kernel, [block(edge)], [VMEM] * 5, flops(edge, 2 * edge))(
        v_o, part_o, *rows_o, corner_far
    )
    f_b, f_all = call(
        last_kernel, [block(edge, BF16), block(owned, BF16)], [VMEM] * 10, edge * width * 8
    )(r_e, r_o, p_e, p_o, scale, y_e, y_o, w_e, w_o, f_m)
    far_b = [shift(f_b, k) for k in range(2, bands)]
    near = shift(f_all, 1)
    (filtered,) = call(join_kernel, [block(owned, BF16)], [VMEM], 1 << 10)(f_all)
    total = bands * width
    (before,) = call(
        margin_m_kernel,
        [((total - 2 * width, width), F32)],
        [VMEM] * (bands - 1),
        2 * total * width * inner,
    )(f_m, *far_m)
    (sums,) = call(
        margin_b_kernel, [((total, width), BF16)], [VMEM] * (bands + 2), 2 * total * width * owned
    )(f_all, near, before, f_b, *far_b)
    parts = lax.all_to_all(sums.reshape(domains, total // domains, width), "dom", 0, 0)
    factor = 1.0 / jnp.sqrt(F32(owned * domains))
    return (filtered, (jnp.sum(parts.astype(F32), axis=0) * factor).T)


def solution(mesh):
    return jax.shard_map(
        shards,
        mesh=mesh,
        in_specs=(P("dom", "band"), P("dom", None, None), P("dom", None), P("dom"), P("dom")),
        out_specs=(P("dom", "band"), P("band", "dom")),
        check_vma=False,
    )
```

```python
import functools

import jax
import jax.numpy as jnp
from jax import lax
from jax.experimental import pallas as pl
from jax.experimental.pallas import tpu as pltpu
from jax.sharding import PartitionSpec as P


DEGREE = 4
LANES = 128
PAD = 16
VMEM_LIMIT = 16 << 20

filter_center = 0.5
filter_halfwidth = 3.0

F32 = jnp.float32
BF16 = jnp.bfloat16
VMEM = pl.BlockSpec(memory_space=pltpu.VMEM)
SMEM = pl.BlockSpec(memory_space=pltpu.SMEM)
HBM = pl.BlockSpec(memory_space=pltpu.HBM)


def call(kernel, outs, ins, flops, scratch=()):
    return pl.pallas_call(
        kernel,
        out_shape=[jax.ShapeDtypeStruct(s, d) for s, d in outs],
        in_specs=ins,
        out_specs=[VMEM] * len(outs),
        scratch_shapes=list(scratch),
        cost_estimate=pl.CostEstimate(flops=flops, bytes_accessed=1 << 20, transcendentals=0),
        compiler_params=pltpu.CompilerParams(vmem_limit_bytes=VMEM_LIMIT),
    )


def is_odd():
    return jnp.bitwise_and(lax.axis_index("dom"), 1) == 1


def at(start, size):
    return pl.ds(pl.multiple_of(start, LANES), size)


def to_columns(row):
    width = row.shape[1]
    parts = [
        jnp.broadcast_to(row[:, i : i + LANES], (LANES, LANES)).T for i in range(0, width, LANES)
    ]
    return parts[0] if len(parts) == 1 else jnp.concatenate(parts, axis=0)


def split(x):
    high = x.astype(BF16)
    return high, (x - high.astype(F32)).astype(BF16)


def dot(a, b):
    return jnp.dot(a, b, preferred_element_type=F32)


def apply(hi_ref, lo_ref, cols, values):
    return dot(hi_ref[:, cols], values) + dot(lo_ref[:, cols], values)


def advance(applied, current, previous):
    moved = (applied - filter_center * current) / filter_halfwidth
    return moved if previous is None else 2.0 * moved - previous


def rim_kernel(
    count_ref, v_hbm, d_hbm, conn_hbm, ham_hbm, ro_ref, re_ref, v_ref, d_ref, pos_ref, ham_ref, sems
):
    pairs = (
        (ham_hbm, ham_ref),
        (v_hbm, v_ref),
        (d_hbm, d_ref),
        (conn_hbm, pos_ref),
    )
    copies = [pltpu.make_async_copy(a, b, sems.at[i]) for i, (a, b) in enumerate(pairs)]
    for copy in copies[1:] + copies[:1]:
        copy.start()
    odd = is_odd()
    owned = v_ref.shape[0]
    g = ro_ref.shape[0] - PAD
    far = owned - g
    row = lax.broadcasted_iota(jnp.int32, (PAD, LANES), 0)
    for copy in copies[1:]:
        copy.wait()
    for out, edge in ((ro_ref, jnp.where(odd, far, 0)), (re_ref, jnp.where(odd, 0, far))):
        out[:g, :] = v_ref[at(edge, g), :]
        mass = d_ref[pl.ds(edge // LANES, 1), :]
        high = mass.astype(BF16).astype(F32)
        out[g:, :] = jnp.where(row == 0, high, jnp.where(row == 1, mass - high, 0.0)).astype(BF16)
    cells, slots = pos_ref.shape
    edge = slots // 2
    base = owned + 2 * g - edge
    conn = pos_ref[...]
    turned = jnp.where(conn < edge, conn + base, jnp.where(conn >= base, conn - base, conn))
    live = lax.broadcasted_iota(jnp.int32, (cells, slots), 0) < count_ref[0]
    pos_ref[...] = jnp.where(live, jnp.where(odd, turned, conn), -1)
    copies[0].wait()


def gather_rows(pos_ref, ham_ref, pick_ref, first, count):
    cells, slots = pos_ref.shape
    total = None
    for c in range(cells):
        row = pos_ref[c : c + 1, :]
        spread = lax.broadcasted_iota(jnp.int32, (count, slots), 0) + first == row
        spread = jnp.where(spread, 1.0, 0.0).astype(BF16)
        high, low = split(dot(spread, ham_ref[c]))
        pick = pick_ref[c * slots : (c + 1) * slots, :]
        part = dot(high, pick) + dot(low, pick)
        total = part if total is None else total + part
    return split(total)


def assemble_om_kernel(pos_ref, ham_ref, ho_ref, lo_ref, hm_ref, lm_ref, pick_ref, corner_ref):
    edge, ext = ho_ref.shape
    inner = hm_ref.shape[0]
    cells, slots = pos_ref.shape
    lane = lax.broadcasted_iota(jnp.int32, (slots, LANES), 1)
    for c in range(cells):
        column = to_columns(pos_ref[c : c + 1, :].astype(F32)).astype(jnp.int32)
        for i in range(0, ext, LANES):
            pick_ref[c * slots : (c + 1) * slots, i : i + LANES] = jnp.where(
                lane + i == column, 1.0, 0.0
            ).astype(BF16)
    high, low = gather_rows(pos_ref, ham_ref, pick_ref, 0, edge + inner)
    ho_ref[...] = high[:edge]
    lo_ref[...] = low[:edge]
    hm_ref[...] = high[edge:]
    lm_ref[...] = low[edge:]
    corner_ref[...] = high[:edge, :edge]


def assemble_e_kernel(pos_ref, ham_ref, pick_ref, he_ref, le_ref):
    edge, ext = he_ref.shape
    he_ref[...], le_ref[...] = gather_rows(pos_ref, ham_ref, pick_ref, ext - edge, edge)


def first_o_kernel(v_ref, he_ref, ho_ref, hi_ref, lo_ref, vx_ref, p_ref, s_ref):
    odd = is_odd()
    owned = v_ref.shape[0]
    ext = hi_ref.shape[1]
    g = (ext - owned) // 2
    base = ext - 2 * g
    far = owned - g
    vx_ref[at(jnp.where(odd, g, 0), g), :] = ho_ref[:g, :]
    vx_ref[at(jnp.where(odd, 0, g), g), :] = v_ref[at(jnp.where(odd, far, 0), g), :]
    vx_ref[2 * g : base, :] = v_ref[g:far, :]
    vx_ref[at(base + jnp.where(odd, 0, g), g), :] = he_ref[:g, :]
    vx_ref[at(base + jnp.where(odd, g, 0), g), :] = v_ref[at(jnp.where(odd, 0, far), g), :]
    product = apply(hi_ref, lo_ref, slice(None), vx_ref[...])
    p_ref[...] = product
    s_ref[...] = product.astype(BF16)


def first_e_kernel(vx_ref, hi_ref, lo_ref, p_ref):
    p_ref[...] = apply(hi_ref, lo_ref, slice(None), vx_ref[...])


def columns(cols, v, rows, outs, before=(None, None, None)):
    for i, (out, part) in enumerate(zip(outs, before)):
        product = apply(rows[2 * i], rows[2 * i + 1], cols, v)
        out[...] = product if part is None else part[...] + product


def inner_columns(v, rows, outs):
    edge = rows[0].shape[0]
    columns(slice(edge, edge + v.shape[0]), v, rows, outs)


def first_m_kernel(vx_ref, he_ref, ho_ref, d_ref, *refs):
    rows, (c_ref, y_out), outs = refs[:6], refs[6:8], refs[8:]
    hm_ref, lm_ref = rows[2:4]
    odd = is_odd()
    ext = hm_ref.shape[1]
    g = he_ref.shape[0] - PAD
    owned = ext - 2 * g
    base = ext - 2 * g
    far = owned - g

    def mass(ref):
        return to_columns(jnp.sum(ref[g:, :].astype(F32), axis=0, keepdims=True))

    def own(block):
        return to_columns(d_ref[pl.ds(block, 1), :])

    c_ref[at(jnp.where(odd, g, 0), g), :] = mass(ho_ref)
    c_ref[at(jnp.where(odd, 0, g), g), :] = own(jnp.where(odd, far // LANES, 0))
    for i in range(1, far // LANES):
        c_ref[g + i * LANES : g + (i + 1) * LANES, :] = own(i)
    c_ref[at(base + jnp.where(odd, 0, g), g), :] = mass(he_ref)
    c_ref[at(base + jnp.where(odd, g, 0), g), :] = own(jnp.where(odd, 0, far // LANES))
    middle = slice(2 * g, base)
    product = apply(hm_ref, lm_ref, slice(None), vx_ref[...])
    y = advance(c_ref[middle, :] * product, vx_ref[middle, :].astype(F32), None)
    y_out[...] = y
    inner_columns(y.astype(BF16), rows, outs)


def even_kernel(first, last, r_ref, p_ref, c_ref, y_ref, *rest):
    rest = list(rest)
    prev_ref = None if first else rest.pop(0)
    before, rows, y_out, outs, s_out = rest[:3], rest[3:9], rest[9], rest[10:13], rest[13]
    ext = rows[0].shape[1]
    edge = r_ref.shape[0]
    block = slice(ext - edge, ext)
    current = y_ref[block, :].astype(F32) if first else y_ref[...]
    previous = None if first else tail(prev_ref, edge)
    y = advance(c_ref[block, :] * (p_ref[...] + r_ref[...]), current, previous)
    y_out[...] = y
    columns(block, y.astype(BF16), rows, outs, before)
    if last:
        g = s_out.shape[0]
        s_out[...] = outs[0][at(jnp.where(is_odd(), g, 0), g), :].astype(BF16)
    else:
        s_out[...] = outs[0][...].astype(BF16)


def tail(ref, size):
    return ref[ref.shape[0] - size :, :].astype(F32)


def head(ref, size):
    return ref[:size, :].astype(F32)


def corner(ho_ref, lo_ref, k_ref, values):
    return apply(ho_ref, lo_ref, slice(0, values.shape[0]), values) + dot(k_ref[...], values)


def odd_kernel(first, r_ref, p_ref, c_ref, y_ref, *rest):
    y_out, v_out = rest[-2:]
    edge = r_ref.shape[0]
    total = p_ref[...] + r_ref[...].astype(F32)
    previous = None if first else head(rest[0], edge)
    y = advance(c_ref[:edge, :] * total, head(y_ref, edge), previous)
    y_out[...] = y
    v_out[...] = y.astype(BF16)


def rest_e_kernel(v_ref, part_ref, he_ref, le_ref, p_out, *s_out):
    edge = v_ref.shape[0]
    p_out[...] = part_ref[...] + apply(he_ref, le_ref, slice(0, edge), v_ref[...])
    if s_out:
        g = s_out[0].shape[0]
        s_out[0][...] = p_out[at(jnp.where(is_odd(), 0, g), g), :]


def next_inner(v_ref, part_ref, c_ref, y_ref, prev_ref, hm_ref, lm_ref):
    ext = hm_ref.shape[1]
    edge = v_ref.shape[0]
    product = part_ref[...] + apply(hm_ref, lm_ref, slice(0, edge), v_ref[...])
    middle = slice(edge, edge + y_ref.shape[0])
    previous = prev_ref[middle, :].astype(F32) if prev_ref.shape[0] == ext else prev_ref[...]
    return advance(c_ref[middle, :] * product, y_ref[...], previous)


def rest_m_kernel(v_ref, part_ref, po_ref, c_ref, y_ref, prev_ref, k_ref, *refs):
    rows, y_out, outs, p_out = refs[:6], refs[6], refs[7:10], refs[10]
    y = next_inner(v_ref, part_ref, c_ref, y_ref, prev_ref, *rows[2:4])
    y_out[...] = y
    inner_columns(y.astype(BF16), rows, outs)
    p_out[...] = po_ref[...] + corner(rows[0], rows[1], k_ref, v_ref[...])


def last_m_kernel(v_ref, part_ref, c_ref, y_ref, prev_ref, hm_ref, lm_ref, f_out):
    f_out[...] = next_inner(v_ref, part_ref, c_ref, y_ref, prev_ref, hm_ref, lm_ref).astype(BF16)


def corner_kernel(v_ref, p_ref, ho_ref, lo_ref, k_ref, p_out):
    p_out[...] = p_ref[...] + corner(ho_ref, lo_ref, k_ref, v_ref[...])


def last_kernel(re_ref, ro_ref, pe_ref, po_ref, c_ref, ye_ref, yo_ref, we_ref, wo_ref, fm_ref, f_ref, all_ref):
    odd = is_odd()
    ext = c_ref.shape[0]
    g = re_ref.shape[0]
    base = ext - 2 * g
    here = at(jnp.where(odd, 0, g), g)
    total = po_ref[here, :] + ro_ref[...].astype(F32)
    f_ref[:g, :] = advance(c_ref[here, :] * total, yo_ref[here, :], wo_ref[here, :]).astype(BF16)
    here = at(jnp.where(odd, g, 0), g)
    total = pe_ref[here, :] + re_ref[...]
    scale = c_ref[at(base + jnp.where(odd, g, 0), g), :]
    f_ref[g:, :] = advance(scale * total, ye_ref[here, :], we_ref[here, :]).astype(BF16)
    inner = fm_ref.shape[0]
    all_ref[:inner, :] = fm_ref[...]
    all_ref[inner:, :] = f_ref[...]


def join_kernel(all_ref, out_ref):
    odd = is_odd()
    g = LANES
    far = out_ref.shape[0] - g
    inner = far - g
    out_ref[g:far, :] = all_ref[:inner, :]
    out_ref[at(jnp.where(odd, far, 0), g), :] = all_ref[inner : inner + g, :]
    out_ref[at(jnp.where(odd, 0, far), g), :] = all_ref[inner + g :, :]


def gram(a, b):
    return lax.dot_general(a, b, (((0,), (0,)), ((), ())), preferred_element_type=F32)


def place(k, width):
    return at((lax.axis_index("band") ^ k) * width, width)


def margin_m_kernel(all_ref, own_ref, *refs):
    out_ref = refs[-1]
    width = own_ref.shape[1]
    last = len(refs) - 1
    out_ref[last * width :, :] = gram(all_ref[...], all_ref[...])
    for i, ref in enumerate(refs[:-1]):
        out_ref[i * width : (i + 1) * width, :] = gram(ref[...], own_ref[...])


def margin_b_kernel(all_ref, near_ref, before_ref, own_ref, *refs):
    out_ref = refs[-1]
    width = own_ref.shape[1]
    out_ref[place(0, width), :] = before_ref[(len(refs) - 1) * width :, :].astype(BF16)
    out_ref[place(1, width), :] = gram(near_ref[...], all_ref[...]).astype(BF16)
    for i, ref in enumerate(refs[:-1]):
        block = before_ref[i * width : (i + 1) * width, :] + gram(ref[...], own_ref[...])
        out_ref[place(i + 2, width), :] = block.astype(BF16)


def shards(wavefunctions, cell_ham, connectivity, inv_mass, cell_count):
    owned, width = wavefunctions.shape
    cells, slots = connectivity.shape
    g = cell_ham.shape[1] // 4
    edge = 2 * g
    ext = owned + edge
    inner = ext - 2 * edge
    domains = lax.axis_size("dom")
    bands = lax.axis_size("band")
    if domains % 2 or bands & (bands - 1) or g != LANES or width != LANES or slots != 2 * edge:
        raise ValueError("unsupported sizes")
    even_pairs = [(i, i ^ 1) for i in range(domains)]
    odd_pairs = [(i, (i + 1) % domains if i % 2 else (i - 1) % domains) for i in range(domains)]

    def swap_even(x):
        return lax.ppermute(x, "dom", even_pairs)

    def swap_odd(x):
        return lax.ppermute(x, "dom", odd_pairs)

    def shift(x, k):
        return lax.ppermute(x, "band", [(i, i ^ k) for i in range(bands)])

    def flops(rows, cols):
        return 4 * rows * cols * width

    masses = inv_mass.reshape(owned // LANES, LANES)
    rim = ((g + PAD, width), BF16)
    inputs = (wavefunctions, masses, connectivity, cell_ham)
    rim_o, rim_e, wavefunctions, masses, position, cell_ham = call(
        rim_kernel,
        [rim, rim] + [(x.shape, x.dtype) for x in inputs],
        [SMEM] + [HBM] * 4,
        1 << 10,
        [pltpu.SemaphoreType.DMA((4,))],
    )(cell_count, *[pltpu.with_memory_space_constraint(x, pltpu.HBM) for x in inputs])
    halo_o = swap_odd(rim_o)
    halo_e = swap_even(rim_e)

    def block(rows, dtype=F32, cols=width):
        return ((rows, cols), dtype)

    *rows_om, pick, corner_mine = call(
        assemble_om_kernel,
        [block(edge, BF16, ext)] * 2
        + [block(inner, BF16, ext)] * 2
        + [block(cells * slots, BF16, ext), block(edge, BF16, edge)],
        [VMEM] * 2,
        2 * cells * (edge + inner) * slots * (slots + 2 * ext),
    )(position, cell_ham)
    rows_o, rows_m = rows_om[:2], rows_om[2:]
    start, p_o, s_o = call(
        first_o_kernel,
        [block(ext, BF16), block(edge), block(edge, BF16)],
        [VMEM] * 5,
        flops(edge, ext),
    )(wavefunctions, halo_e, halo_o, *rows_o)
    r_o = swap_odd(s_o)
    corner_far = lax.ppermute(corner_mine, "dom", odd_pairs)
    rows_e = call(
        assemble_e_kernel,
        [block(edge, BF16, ext)] * 2,
        [VMEM] * 3,
        2 * cells * edge * slots * (slots + 2 * ext),
    )(position, cell_ham, pick)
    rows = (*rows_o, *rows_m, *rows_e)

    (p_e,) = call(first_e_kernel, [block(edge)], [VMEM] * 3, flops(edge, ext))(start, *rows_e)
    s_e = p_e
    thirds = [block(edge), block(inner), block(edge)]
    y_e = y_o = w_m = start
    w_e = w_o = v_o = y_m = part_o = part_m = part_e = None
    for step in range(1, DEGREE):
        last = step == DEGREE - 1
        first = step == 1
        r_e = swap_even(s_e)
        if first:
            scale, y_m, *middle = call(
                first_m_kernel, [block(ext), block(inner)] + thirds, [VMEM] * 10, flops(ext, ext)
            )(start, halo_e, halo_o, masses, *rows)
        else:
            new_m, *middle, p_o = call(
                rest_m_kernel, [block(inner)] + thirds + [block(edge)], [VMEM] * 13, flops(ext, ext)
            )(v_o, part_m, part_o, scale, y_m, w_m, corner_far, *rows)
            w_m, y_m = y_m, new_m
        new_e, part_o, part_m, part_e, s_o = call(
            functools.partial(even_kernel, first, last),
            [block(edge)] + thirds + [block(g if last else edge, BF16)],
            [VMEM] * (13 if first else 14),
            flops(ext, edge),
        )(r_e, p_e, scale, y_e, *(() if first else (w_e,)), *middle, *rows)
        r_next = swap_odd(s_o)
        new_o, v_o = call(
            functools.partial(odd_kernel, first),
            [block(edge), block(edge, BF16)],
            [VMEM] * (4 if first else 5),
            1 << 10,
        )(r_o, p_o, scale, y_o, *(() if first else (w_o,)))
        p_e, *half = call(
            rest_e_kernel, [block(edge)] + [block(g)] * last, [VMEM] * 4, flops(edge, edge)
        )(v_o, part_e, *rows_e)
        s_e = half[0] if last else p_e
        r_o = r_next
        w_e, w_o = y_e, y_o
        y_e, y_o = new_e, new_o
    r_e = swap_even(s_e)
    (f_m,) = call(last_m_kernel, [block(inner, BF16)], [VMEM] * 7, flops(inner, edge))(
        v_o, part_m, scale, y_m, w_m, *rows_m
    )
    far_m = [shift(f_m, k) for k in range(2, bands)]
    (p_o,) = call(corner_kernel, [block(edge)], [VMEM] * 5, flops(edge, 2 * edge))(
        v_o, part_o, *rows_o, corner_far
    )
    f_b, f_all = call(
        last_kernel, [block(edge, BF16), block(owned, BF16)], [VMEM] * 10, edge * width * 8
    )(r_e, r_o, p_e, p_o, scale, y_e, y_o, w_e, w_o, f_m)
    far_b = [shift(f_b, k) for k in range(2, bands)]
    near = shift(f_all, 1)
    (filtered,) = call(join_kernel, [block(owned, BF16)], [VMEM], 1 << 10)(f_all)
    total = bands * width
    (before,) = call(
        margin_m_kernel, [((total - width, width), F32)], [VMEM] * bands, 2 * total * width * inner
    )(f_all, f_m, *far_m)
    (sums,) = call(
        margin_b_kernel, [((total, width), BF16)], [VMEM] * (bands + 2), 2 * total * width * owned
    )(f_all, near, before, f_b, *far_b)
    parts = lax.all_to_all(sums.reshape(domains, total // domains, width), "dom", 0, 0)
    factor = 1.0 / jnp.sqrt(F32(owned * domains))
    return (filtered, (jnp.sum(parts.astype(F32), axis=0) * factor).T)


def solution(mesh):
    return jax.shard_map(
        shards,
        mesh=mesh,
        in_specs=(P("dom", "band"), P("dom", None, None), P("dom", None), P("dom"), P("dom")),
        out_specs=(P("dom", "band"), P("band", "dom")),
        check_vma=False,
    )
```
